32 devices in a mesh: shard: 2 (over x), ctx: 4 (over y, core), tp: 4 (over z).
Axes of the slice: x: 2, y: 2, z: 4, core: 2. Of those that a mesh axis runs over, the one named last changes fastest.
Arguments:
- tokens: bfloat16 [6, 608, 1024], P('shard', 'ctx'), may hold values from -6 to 6
- pad_mask: int32 [6, 608], P('shard', 'ctx'), may hold values from 0 to 1, as said below
- ln1_gain: float32 [1024], replicated, may hold values from 0.25 to 1.75
- ln1_shift: float32 [1024], replicated, may hold values from -3 to 3
- w_qkv: bfloat16 [3, 1024, 1024], P(None, 'shard', 'tp'), may hold values from -0.1875 to 0.1875
- b_qv: float32 [2, 1024], P(None, 'tp'), may hold values from -3 to 3
- w_out: bfloat16 [1024, 1024], P('tp', 'shard'), may hold values from -1 to 1
- b_out: float32 [1024], replicated, may hold values from -3 to 3
- ln2_gain: float32 [1024], replicated, may hold values from 0.25 to 1.75
- ln2_shift: float32 [1024], replicated, may hold values from -3 to 3
- w_up: bfloat16 [1024, 4096], P('shard', 'tp'), may hold values from -0.1875 to 0.1875
- b_up: float32 [4096], P('tp'), may hold values from -3 to 3
- w_down: bfloat16 [4096, 1024], P('tp', 'shard'), may hold values from -0.09375 to 0.09375
- b_down: float32 [1024], replicated, may hold values from -4 to 4
- cotangent: bfloat16 [6, 608, 1024], P('shard', 'ctx'), may hold values from -6 to 6
Outputs:
- out_tokens: float32 [6, 608, 1024], P('shard', 'ctx')
- grad_tokens: float32 [6, 608, 1024], P('shard', 'ctx')
- grad_w_qkv: float32 [3, 1024, 1024], P(None, 'shard', 'tp')
- grad_b_qv: float32 [2, 1024], P(None, 'tp')
- grad_w_out: float32 [1024, 1024], P('tp', 'shard')
- grad_b_out: float32 [1024], replicated
- grad_ln1_gain: float32 [1024], replicated
- grad_ln1_shift: float32 [1024], replicated
- grad_ln2_gain: float32 [1024], replicated
- grad_ln2_shift: float32 [1024], replicated
- grad_w_up: float32 [1024, 4096], P('shard', 'tp')
- grad_b_up: float32 [4096], P('tp')
- grad_w_down: float32 [4096, 1024], P('tp', 'shard')
- grad_b_down: float32 [1024], replicated
The draws below stay inside these ranges and needn't reach their ends.
Inputs may be any that keep to these rules, and one draw needn't show every extreme that they name: `pad_mask`: each image has exactly 577 ones; the 31 padding slots may lie anywhere in the image.
All inputs are finite; a program needn't handle non-finite values.
Results may differ from the reference program's by a relative error of at most 0.02.
Values may be sent and summed in bfloat16 or wider, within the bound.
A program may use at most 128 MiB of HBM per device.

```python
import math
import jax
import jax.numpy as jnp
from jax import lax

D = 1024
HEADS = 16
HD = 64
FF = 4096
VALID = 577
SEQ = 608
IMAGES = 6
N_TP = 4


def draw_pad_mask(key, part):
    image_keys = jax.random.split(key, IMAGES)

    def one_image(image_key):
        order = jax.random.permutation(image_key, SEQ)
        return (order < VALID).astype(jnp.int32)
    return jax.vmap(one_image)(image_keys)


def steps_of(rng, dims, cuts, least, top_value):
    def one(dim, blocks):
        draws = jax.random.uniform(jax.random.fold_in(jax.random.fold_in(rng, 6), dim), (blocks,), jnp.float32, least / len(cuts), top_value / len(cuts))
        return jnp.repeat(jnp.exp(draws), dims[dim] // blocks).reshape((-1,) + (1,) * (len(dims) - dim - 1))

    level = one(*cuts[0])
    for cut in cuts[1:]:
        level = level * one(*cut)
    return level


def noise(key, extent, spread, reach, shards=(), held_as=jnp.bfloat16):
    drawn = spread * jax.random.normal(key, extent, jnp.float32)
    if shards:
        drawn = drawn * steps_of(key, extent, shards, -0.22, 0.18)
    return jnp.clip(drawn, -reach, reach).astype(held_as)


def setup_inputs(seed: int = 0) -> dict:
    keys = jax.random.split(jax.random.key(seed), 16)
    tokens = noise(keys[0], (IMAGES, SEQ, D), 1.0, 6.0, ((0, 2), (1, 4)))
    pad_mask = draw_pad_mask(jax.random.fold_in(keys[15], 71), 0)
    ln1_gain = jnp.clip(1.0 + 0.15 * jax.random.normal(keys[2], (D,), jnp.float32), 0.25, 1.75)
    ln1_shift = noise(keys[3], (D,), 0.5, 3.0, (), jnp.float32)
    w_qkv = noise(keys[4], (3, D, D), D ** -0.5, 0.1875, ((1, 2), (2, 4)))
    b_qv = noise(keys[5], (2, D), 0.5, 3.0, ((1, 4),), jnp.float32)
    w_out = noise(keys[6], (D, D), (D // 24) ** -0.5, 1.0, ((0, 4), (1, 2)))
    b_out = noise(keys[7], (D,), 0.5, 3.0, (), jnp.float32)
    ln2_gain = jnp.clip(1.0 + 0.15 * jax.random.normal(keys[8], (D,), jnp.float32), 0.25, 1.75)
    ln2_shift = noise(keys[9], (D,), 0.5, 3.0, (), jnp.float32)
    w_up = noise(keys[10], (D, FF), D ** -0.5, 0.1875, ((0, 2), (1, 4)))
    b_up = noise(keys[11], (FF,), 0.5, 3.0, ((0, 4),), jnp.float32)
    w_down = noise(keys[12], (FF, D), FF ** -0.5, 0.09375, ((0, 4), (1, 2)))
    b_down = noise(keys[13], (D,), 1.0, 4.0, (), jnp.float32)
    cotangent = noise(keys[14], (IMAGES, SEQ, D), 1.0, 6.0, ((0, 2), (1, 4)))
    return dict(tokens=tokens, pad_mask=pad_mask, ln1_gain=ln1_gain, ln1_shift=ln1_shift, w_qkv=w_qkv, b_qv=b_qv, w_out=w_out, b_out=b_out, ln2_gain=ln2_gain, ln2_shift=ln2_shift, w_up=w_up, b_up=b_up, w_down=w_down, b_down=b_down, cotangent=cotangent)


NEG_FILL = -1e+30

def normalize(values, gain, shift):
    row_mean = lax.optimization_barrier(jnp.mean(values, axis=-1, keepdims=True))
    centred = values - row_mean
    inv_std = lax.rsqrt(lax.optimization_barrier(jnp.mean(centred * centred, axis=-1, keepdims=True)) + 1e-06)
    unit_rows = centred * inv_std
    return (unit_rows, inv_std, unit_rows * gain + shift)

def norm_back(upstream, unit_rows, inv_std, gain):
    scaled = upstream * gain
    centre = lax.optimization_barrier(jnp.mean(scaled, axis=-1, keepdims=True))
    along = lax.optimization_barrier(jnp.mean(scaled * unit_rows, axis=-1, keepdims=True))
    return inv_std * (scaled - centre - unit_rows * along)

def gelu_slope(pre_act):
    return 0.5 * (1.0 + lax.erf(pre_act * 0.7071067811865476)) + pre_act * jnp.exp(-0.5 * pre_act * pre_act) * 0.3989422804014327

def grouped_sum(left, right):
    tok_count, stack_count, inner = left.shape
    width = inner // N_TP
    left_parts = left.reshape(tok_count, stack_count, N_TP, width).astype(jnp.float32)
    right_parts = right.reshape(stack_count, N_TP, width, right.shape[-1]).astype(jnp.float32)
    partial_sums = jnp.einsum('tcgw,cgwd->gtd', left_parts, right_parts)
    rounded = lax.optimization_barrier(partial_sums.astype(jnp.bfloat16))
    return lax.optimization_barrier(jnp.sum(rounded.astype(jnp.float32), axis=0))

def reference(tokens, pad_mask, ln1_gain, ln1_shift, w_qkv, b_qv, w_out, b_out, ln2_gain, ln2_shift, w_up, b_up, w_down, b_down, cotangent):
    scale = 1.0 / math.sqrt(HD)

    def one_image(totals, item):
        image, valid, upstream = item
        inputs_wide = image.astype(jnp.float32)
        first_unit, first_inv, first_norm = normalize(inputs_wide, ln1_gain, ln1_shift)
        first_low = first_norm.astype(jnp.bfloat16)
        projected = jnp.einsum('td,cdh->cth', first_low.astype(jnp.float32), w_qkv.astype(jnp.float32))
        queries = (projected[0] + b_qv[0]).astype(jnp.bfloat16).reshape(SEQ, HEADS, HD)
        key_heads = projected[1].astype(jnp.bfloat16).reshape(SEQ, HEADS, HD)
        value_heads = (projected[2] + b_qv[1]).astype(jnp.bfloat16).reshape(SEQ, HEADS, HD)
        scores = jnp.einsum('qhe,khe->hqk', queries.astype(jnp.float32), key_heads.astype(jnp.float32)) * scale
        scores = jnp.where(valid[None, None, :] > 0, scores, NEG_FILL)
        row_top = lax.optimization_barrier(jnp.max(scores, axis=-1, keepdims=True))
        log_total = row_top + jnp.log(lax.optimization_barrier(jnp.sum(jnp.exp(scores - row_top), axis=-1, keepdims=True)))
        weights = jnp.exp(scores - log_total)
        weights_low = weights.astype(jnp.bfloat16)
        attended = jnp.einsum('hqk,khe->qhe', weights_low.astype(jnp.float32), value_heads.astype(jnp.float32)).astype(jnp.bfloat16).reshape(SEQ, D)
        middle = inputs_wide + grouped_sum(attended[:, None, :], w_out[None]) + b_out
        second_unit, second_inv, second_norm = normalize(middle, ln2_gain, ln2_shift)
        second_low = second_norm.astype(jnp.bfloat16)
        pre_act = jnp.dot(second_low, w_up, preferred_element_type=jnp.float32) + b_up
        activated = jax.nn.gelu(pre_act, approximate=False).astype(jnp.bfloat16)
        result = middle + grouped_sum(activated[:, None, :], w_down[None]) + b_down
        upstream_wide = upstream.astype(jnp.float32)
        act_grad = jnp.dot(upstream, w_down.T, preferred_element_type=jnp.float32) * gelu_slope(pre_act)
        act_low = act_grad.astype(jnp.bfloat16)
        grad_down = jnp.dot(activated.T, upstream, preferred_element_type=jnp.float32)
        grad_up = jnp.dot(second_low.T, act_low, preferred_element_type=jnp.float32)
        norm2_grad = grouped_sum(act_low[:, None, :], w_up.T[None])
        middle_grad = upstream_wide + norm_back(norm2_grad, second_unit, second_inv, ln2_gain)
        middle_low = middle_grad.astype(jnp.bfloat16)
        grad_out = jnp.dot(attended.T, middle_low, preferred_element_type=jnp.float32)
        attended_grad = jnp.dot(middle_low, w_out.T, preferred_element_type=jnp.float32).astype(jnp.bfloat16).reshape(SEQ, HEADS, HD)
        weight_grad = jnp.einsum('qhe,khe->hqk', attended_grad.astype(jnp.float32), value_heads.astype(jnp.float32))
        row_dot = lax.optimization_barrier(jnp.sum(weights * weight_grad, axis=-1, keepdims=True))
        score_grad = (scale * weights * (weight_grad - row_dot)).astype(jnp.bfloat16)
        query_grad = jnp.einsum('hqk,khe->qhe', score_grad.astype(jnp.float32), key_heads.astype(jnp.float32)).reshape(SEQ, D)
        key_grad = jnp.einsum('hqk,qhe->khe', score_grad.astype(jnp.float32), queries.astype(jnp.float32)).reshape(SEQ, D)
        value_grad = jnp.einsum('hqk,qhe->khe', weights_low.astype(jnp.float32), attended_grad.astype(jnp.float32)).reshape(SEQ, D)
        proj_grad = jnp.stack([query_grad, key_grad, value_grad]).astype(jnp.bfloat16)
        grad_qkv = jnp.einsum('td,cth->cdh', first_low.astype(jnp.float32), proj_grad.astype(jnp.float32))
        norm1_grad = grouped_sum(proj_grad.transpose(1, 0, 2), w_qkv.transpose(0, 2, 1))
        input_grad = middle_grad + norm_back(norm1_grad, first_unit, first_inv, ln1_gain)
        pieces = (grad_qkv, jnp.stack([lax.optimization_barrier(jnp.sum(query_grad, axis=0)), lax.optimization_barrier(jnp.sum(value_grad, axis=0))]), grad_out, lax.optimization_barrier(jnp.sum(middle_grad, axis=0)), lax.optimization_barrier(jnp.sum(norm1_grad * first_unit, axis=0)), lax.optimization_barrier(jnp.sum(norm1_grad, axis=0)), lax.optimization_barrier(jnp.sum(norm2_grad * second_unit, axis=0)), lax.optimization_barrier(jnp.sum(norm2_grad, axis=0)), grad_up, lax.optimization_barrier(jnp.sum(act_grad, axis=0)), grad_down, lax.optimization_barrier(jnp.sum(upstream_wide, axis=0)))
        totals = jax.tree.map(jnp.add, totals, pieces)
        return (totals, (result, input_grad))
    start = (jnp.zeros((3, D, D), jnp.float32), jnp.zeros((2, D), jnp.float32), jnp.zeros((D, D), jnp.float32), jnp.zeros((D,), jnp.float32), jnp.zeros((D,), jnp.float32), jnp.zeros((D,), jnp.float32), jnp.zeros((D,), jnp.float32), jnp.zeros((D,), jnp.float32), jnp.zeros((D, FF), jnp.float32), jnp.zeros((FF,), jnp.float32), jnp.zeros((FF, D), jnp.float32), jnp.zeros((D,), jnp.float32))
    totals, stacked = lax.scan(one_image, start, (tokens, pad_mask, cotangent))
    return (stacked[0], stacked[1], totals[0], totals[1], totals[2], totals[3], totals[4], totals[5], totals[6], totals[7], totals[8], totals[9], totals[10], totals[11])
```

```python
import functools
import math
import types

import jax
import jax.numpy as jnp
from jax import lax
from jax.experimental import pallas as pl
from jax.experimental.pallas import tpu as pltpu
from jax.sharding import PartitionSpec as P

HD = 64
BIG = 1e30
MESH = pl.DeviceIdType.MESH
BF, F32 = jnp.bfloat16, jnp.float32
RB = 32
TILE = 256


def dot(a, b):
    return lax.dot_general(a, b, (((1,), (0,)), ((), ())), preferred_element_type=F32)


def dot_nt(a, b):
    return lax.dot_general(a, b, (((1,), (1,)), ((), ())), preferred_element_type=F32)


def dot_tn(a, b):
    return lax.dot_general(a, b, (((0,), (0,)), ((), ())), preferred_element_type=F32)


def norm_stats(x):
    centred = x - jnp.mean(x, axis=-1, keepdims=True)
    inv = lax.rsqrt(jnp.mean(centred * centred, axis=-1, keepdims=True) + 1e-06)
    return centred * inv, inv


def norm_back(upstream, unit, inv, gain):
    scaled = upstream * gain
    centre = jnp.mean(scaled, axis=-1, keepdims=True)
    along = jnp.mean(scaled * unit, axis=-1, keepdims=True)
    return inv * (scaled - centre - unit * along)


def fold8(x):
    return jnp.sum(x.reshape(x.shape[0] // 8, 8, x.shape[1]), axis=0)


def aligned(i, m):
    return pl.multiple_of(i, m)


class Dims:
    pass


def dims_of(mesh, tokens, w_out, w_up):
    d = Dims()
    d.S, d.C, d.T = (mesh.shape[a] for a in ("shard", "ctx", "tp"))
    assert d.C == 4 and d.T == 4
    d.images, d.piece, d.width = tokens
    d.rows = -(-d.piece // RB) * RB
    d.part = d.width // d.S
    d.local = w_out[0]
    d.hidden = w_up[1]
    d.heads = d.local // HD
    d.keys = d.C * d.rows
    return d


KV, Q, OUT, UP, DN, QKV = range(6)


def scratch_of(d):
    I, R, D, W, F, S, C = d.images, d.rows, d.width, d.local, d.hidden, d.S, d.C
    bf = lambda *shape: pltpu.VMEM(shape, BF)
    f32 = lambda *shape: pltpu.VMEM(shape, F32)
    scratch = dict(
        tok=bf(I, R, D),
        cot=bf(I, R, D),
        maskw=f32(8, TILE),
        first=bf(I, R, D),
        wqkv=bf(3, D, W),
        wout=bf(W, D),
        wup=bf(D, F),
        wdn=bf(F, D),
        q=bf(I, R, W),
        kv=bf(C, I, 2, R, W),
        wts=bf(I, d.heads * R, d.keys),
        att=bf(I, R, W),
        middle=f32(I, R, D),
        second=bf(I, R, D),
        activ=bf(I, R, F),
        actlow=bf(I, R, F),
        mgrad=f32(I, R, D),
        mlow=bf(I, R, D),
        dss=bf(d.heads * R, d.keys),
        qst=bf(d.heads * R, W),
        ost=bf(d.heads * R, W),
        dkv=bf(C, I, 2, R, W),
        rxa=bf(2, I, 2, R, W),
        rxb=bf(I, 2, R, W),
        pg=bf(3, I, R, W),
        acc=f32(8, 8, D),
        sm=f32(8, D),
        smx=f32(S * C, 8, D),
        gqkv=bf(3, D, W),
        gout=bf(W, D),
        gup=bf(D, F),
        gdn=bf(F, D),
        r1qkv=bf(3, D, W // 2),
        r1out=bf(W // 2, D),
        r1up=bf(D, F // 2),
        r1dn=bf(F // 2, D),
        r2qkv=bf(S, 3, D // S, W // 2),
        r2out=bf(S, W // 2, D // S),
        r2up=bf(S, D // S, F // 2),
        r2dn=bf(S, F // 2, D // S),
        r3qkv=bf(3, D // S, W // 2),
        r3out=bf(W // 2, D // S),
        r3up=bf(D // S, F // 2),
        r3dn=bf(F // 2, D // S),
    )
    full = lambda: bf(I, R, D)
    scratch.update(own1=full(), own2=full(), own3=full(), own4=full())
    scratch.update(tot1=full(), tot2=full(), tot3=full(), tot4=full())
    scratch.update(in01=full(), in02=full(), in03=full())
    scratch.update(in11=full(), in12=full(), in13=full())
    scratch["ssem"] = pltpu.SemaphoreType.DMA((MAX_COPIES * S // 2,))
    scratch["rsem"] = pltpu.SemaphoreType.DMA((MAX_COPIES * S // 2,))
    scratch["lsem"] = pltpu.SemaphoreType.DMA((64,))
    return scratch


MAX_COPIES = 200


class Net:
    def __init__(self, ssem, rsem, lsem):
        self.ssem, self.rsem, self.lsem = ssem, rsem, lsem
        self.n = self.m = 0
        self.sent = []
        self.stored = []

    def remote(self, src, dst, device):
        i, self.n = self.n, self.n + 1
        return pltpu.make_async_remote_copy(
            src_ref=src,
            dst_ref=dst,
            send_sem=self.ssem.at[i],
            recv_sem=self.rsem.at[i],
            device_id=device,
            device_id_type=MESH,
        )

    def local(self, src, dst):
        i, self.m = self.m, self.m + 1
        return pltpu.make_async_copy(src, dst, self.lsem.at[i])


def body_kernel(d, names, *refs):
    r = types.SimpleNamespace(**dict(zip(names, refs)))
    I, R, D, W, F, S, C = d.images, d.rows, d.width, d.local, d.hidden, d.S, d.C
    piece, part, heads, keys = d.piece, d.part, d.heads, d.keys
    s, c, t = lax.axis_index("shard"), lax.axis_index("ctx"), lax.axis_index("tp")
    core = lax.rem(c, 2)
    mate = c + 1 - 2 * core
    across = lax.rem(c + 2, 4)
    far = lax.rem(mate + 2, 4)
    tmate = t + 1 - 2 * lax.rem(t, 2)
    tpeer = 3 - t
    inner = lax.rem(t + 1, 4) >= 2
    edge = lax.rem(t + 1, 4) < 2
    on_mate, on_across = (s, mate, t), (s, across, t)
    net = Net(r.ssem, r.rsem, r.lsem)
    sent = net.sent

    def go(copy):
        copy.start()
        sent.append((None, copy))

    loads = {}
    for i in range(I):
        loads["tok", i] = net.local(r.tok_h.at[i], r.tok.at[i, pl.ds(0, piece)])
    rows_s = pl.ds(aligned(s * part, part), part)
    loads[KV] = net.local(r.wqkv_h.at[pl.ds(1, 2)], r.wqkv.at[pl.ds(1, 2), rows_s])
    loads[Q] = net.local(r.wqkv_h.at[pl.ds(0, 1)], r.wqkv.at[pl.ds(0, 1), rows_s])
    loads[OUT] = net.local(r.wout_h, r.wout.at[:, rows_s])
    loads[UP] = net.local(r.wup_h, r.wup.at[rows_s])
    loads[DN] = net.local(r.wdn_h, r.wdn.at[:, rows_s])
    for i in range(I):
        loads["cot", i] = net.local(r.cot_h.at[i], r.cot.at[i, pl.ds(0, piece)])
    for copy in loads.values():
        copy.start()

    barrier = pltpu.get_barrier_semaphore()
    for ds in range(S):
        for dc in range(C):
            if ds or dc:
                where = (lax.rem(s + ds, S), lax.rem(c + dc, C), t)
                pl.semaphore_signal(barrier, inc=1, device_id=where, device_id_type=MESH)
    pl.semaphore_signal(barrier, inc=1, device_id=(s, c, tmate), device_id_type=MESH)

    @pl.when(inner)
    def _():
        pl.semaphore_signal(barrier, inc=1, device_id=(s, c, tpeer), device_id_type=MESH)
        pl.semaphore_wait(barrier, S * C + 1)

    @pl.when(edge)
    def _():
        pl.semaphore_wait(barrier, S * C)

    def half_of(name, ref, shard, half):
        rows = pl.ds(aligned(shard * part, part), part)
        if name in (KV, Q):
            planes = pl.ds(1, 2) if name == KV else pl.ds(0, 1)
            return ref.at[planes, rows, pl.ds(aligned(half * (W // 2), W // 2), W // 2)]
        if name == OUT:
            return ref.at[pl.ds(aligned(half * (W // 2), W // 2), W // 2), rows]
        if name == UP:
            return ref.at[rows, pl.ds(aligned(half * (F // 2), F // 2), F // 2)]
        return ref.at[pl.ds(aligned(half * (F // 2), F // 2), F // 2), rows]

    def own_half(name, ref, half):
        if name in (KV, Q):
            planes = pl.ds(1, 2) if name == KV else pl.ds(0, 1)
            return ref.at[planes, :, pl.ds(aligned(half * (W // 2), W // 2), W // 2)]
        if name == OUT:
            return ref.at[pl.ds(aligned(half * (W // 2), W // 2), W // 2), :]
        if name == UP:
            return ref.at[:, pl.ds(aligned(half * (F // 2), F // 2), F // 2)]
        return ref.at[pl.ds(aligned(half * (F // 2), F // 2), F // 2), :]

    weights = {
        KV: (r.wqkv_h, r.wqkv),
        Q: (r.wqkv_h, r.wqkv),
        OUT: (r.wout_h, r.wout),
        UP: (r.wup_h, r.wup),
        DN: (r.wdn_h, r.wdn),
    }
    gather, spread = {}, {}
    for name, (source, full) in weights.items():
        for ds in range(1, S):
            to = (lax.rem(s + ds, S), c, t)
            copy = net.remote(
                own_half(name, source, core), half_of(name, full, s, core), to
            )
            go(copy)
            gather[name, ds] = copy
            owner = lax.rem(s + S - ds, S)
            held = half_of(name, full, owner, core)
            spread[name, ds] = net.remote(held, held, on_mate)

    def pass_on(name):
        for ds in range(1, S):
            gather[name, ds].wait_recv()
            go(spread[name, ds])

    def weight_ready(name):
        loads[name].wait()
        for ds in range(1, S):
            spread[name, ds].wait_recv()

    tail = piece // 16 * 16

    def clear_tail(ref, i):
        if tail < R:
            old = ref[i, pl.ds(tail, R - tail), :].astype(F32)
            row = lax.broadcasted_iota(jnp.int32, old.shape, 0)
            ref[i, pl.ds(tail, R - tail), :] = jnp.where(row < piece - tail, old, 0.0).astype(BF)

    def blocks(fn):
        def step(b, _):
            fn(pl.ds(aligned(b * RB, RB), RB))
            return 0

        lax.fori_loop(0, R // RB, step, 0)

    def tiles(n, fn):
        def step(b, _):
            fn(pl.ds(aligned(b * TILE, TILE), TILE))
            return 0

        lax.fori_loop(0, n // TILE, step, 0)

    r.acc[...] = jnp.zeros_like(r.acc)
    r.sm[...] = jnp.zeros_like(r.sm)
    r.maskw[...] = jnp.zeros_like(r.maskw)
    r.maskw[0:I, 0:piece] = (r.mask[...] > 0).astype(F32)

    def first_norm(i):
        loads["tok", i].wait()
        clear_tail(r.tok, i)

        def rows(w):
            unit, _ = norm_stats(r.tok[i, w, :].astype(F32))
            r.first[i, w, :] = (unit * r.g1[...] + r.b1[...]).astype(BF)

        blocks(rows)

    for i in range(I):
        first_norm(i)
    pass_on(KV)
    weight_ready(KV)

    kv_mate, kv_across, kv_far = {}, {}, {}
    row_w = lax.broadcasted_iota(jnp.int32, (R, W), 0)

    def keys_values(i):
        x = r.first[i]
        key = dot(x, r.wqkv[1])
        flags = jnp.broadcast_to(r.maskw[i : i + 1, :], (R, W))
        r.kv[c, i, 0] = jnp.where(row_w == piece, flags, key).astype(BF)
        r.kv[c, i, 1] = (dot(x, r.wqkv[2]) + r.bqv[1:2, :]).astype(BF)
        mine = r.kv.at[c, i]
        kv_across[i] = net.remote(mine, mine, on_across)
        kv_mate[i] = net.remote(mine, mine, on_mate)
        theirs = r.kv.at[across, i]
        kv_far[i] = net.remote(theirs, theirs, on_mate)
        go(kv_across[i])
        go(kv_mate[i])

    for i in range(I):
        keys_values(i)
    pass_on(Q)
    weight_ready(Q)
    for i in range(I):
        r.q[i] = (dot(r.first[i], r.wqkv[0]) + r.bqv[0:1, :]).astype(BF)
    pass_on(OUT)

    lane_head = lax.broadcasted_iota(jnp.int32, (R, W), 1) // HD
    scale = 1.0 / math.sqrt(HD)

    def all_keys(i):
        k = jnp.concatenate([r.kv[b, i, 0] for b in range(C)], axis=0)
        v = jnp.concatenate([r.kv[b, i, 1] for b in range(C)], axis=0)
        return k, v

    def key_bias(i):
        row = lax.broadcasted_iota(jnp.int32, (R, W), 0)
        lane = lax.broadcasted_iota(jnp.int32, (R, W), 1)
        lane1 = lax.broadcasted_iota(jnp.int32, (R, 128), 1)
        columns = []
        for b in range(C):
            low = r.kv[b, i, 0, pl.ds(tail, 16), :].astype(F32)
            flags = low[piece - tail : piece - tail + 1, :]
            flag = jnp.sum(jnp.where(row == lane, flags, 0.0), axis=1, keepdims=True)
            columns.append(jnp.where(lane1 == 0, (flag - 1.0) * BIG, 0.0).astype(BF))
        pick = lax.broadcasted_iota(jnp.int32, (16, 128), 1)
        pick = jnp.where(pick == 0, 1.0, 0.0).astype(BF)
        return dot_nt(pick, jnp.concatenate(columns, axis=0))[0:1, :]

    def attention(i):
        kv_far[i].wait_recv()
        kv_mate[i].wait_recv()
        k, v = all_keys(i)
        bias = key_bias(i)
        q = r.q[i].astype(F32)

        def head(h, total):
            mine = lane_head == h
            qh = jnp.where(mine, q, 0.0).astype(BF)
            scores = dot_nt(qh, k) * scale + bias
            top = jnp.max(scores, axis=-1, keepdims=True)
            e = jnp.exp(scores - top)
            w = (e * (1.0 / jnp.sum(e, axis=-1, keepdims=True))).astype(BF)
            r.wts[i, pl.ds(aligned(h * R, R), R), :] = w
            return jnp.where(mine, dot(w, v), total)

        total = lax.fori_loop(0, heads, head, jnp.zeros((R, W), F32))
        r.att[i] = total.astype(BF)

    H = 2
    halves = [pl.ds(j * (R // H), R // H) for j in range(H)]
    hop0, hop1, hop2 = {}, {}, {}

    def sum_plan(k, i):
        own = (r.own1, r.own2, r.own3, r.own4)[k - 1]
        tot = (r.tot1, r.tot2, r.tot3, r.tot4)[k - 1]
        in0 = (r.in01, r.in02, r.in03, r.in01)[k - 1]
        in1 = (r.in11, r.in12, r.in13, r.in11)[k - 1]
        for j, w in enumerate(halves):
            hop0[k, i, j] = net.remote(own.at[i, w], in0.at[i, w], (s, c, tmate))
            hop1[k, i, j] = net.remote(own.at[i, w], in1.at[i, w], (s, c, tpeer))
            hop2[k, i, j] = net.remote(tot.at[i, w], tot.at[i, w], (s, c, tmate))
        return own, tot, in0, in1

    sums = {(k, i): sum_plan(k, i) for k in range(1, 5) for i in range(I)}

    def add_rows(dst, a, b, i, j):
        def step(n, _):
            w = pl.ds(aligned(j * (R // H) + n * 16, 16), 16)
            dst[i, w, :] = (a[i, w, :].astype(F32) + b[i, w, :].astype(F32)).astype(BF)
            return 0

        lax.fori_loop(0, R // H // 16, step, 0)

    def sum_start(k, i):
        @pl.when(edge)
        def _():
            for j in range(H):
                hop0[k, i, j].start()

    def sum_mid(k, i):
        own, tot, in0, in1 = sums[k, i]

        @pl.when(inner)
        def _():
            for j in range(H):
                hop0[k, i, j].wait_recv()
                add_rows(own, own, in0, i, j)
                hop1[k, i, j].start()

    def sum_end(k, i):
        own, tot, in0, in1 = sums[k, i]

        @pl.when(inner)
        def _():
            for j in range(H):
                hop1[k, i, j].wait_recv()
                add_rows(tot, own, in1, i, j)
                hop2[k, i, j].start()

        @pl.when(edge)
        def _():
            for j in range(H):
                hop2[k, i, j].wait_recv()

    def attn_part(i):
        def tile(w):
            r.own1[i, :, w] = dot(r.att[i], r.wout[:, w]).astype(BF)

        tiles(D, tile)

    for i in range(I):
        kv_across[i].wait_recv()
        go(kv_far[i])
    weight_ready(OUT)
    for i in range(I):
        attention(i)
        attn_part(i)
        sum_start(1, i)
        if i:
            sum_mid(1, i - 1)
    sum_mid(1, I - 1)
    pass_on(UP)
    pass_on(DN)
    for i in range(I):
        loads["cot", i].wait()
        clear_tail(r.cot, i)

    def middle_of(i):
        def rows(w):
            x = r.tok[i, w, :].astype(F32) + r.tot1[i, w, :].astype(F32) + r.bout[...]
            r.middle[i, w, :] = x
            unit, _ = norm_stats(x)
            r.second[i, w, :] = (unit * r.g2[...] + r.b2[...]).astype(BF)

        blocks(rows)

    def feed_forward(i):
        def tile(w):
            u = dot(r.second[i], r.wup[:, w]) + r.bup[:, w]
            phi = 0.5 * (1.0 + lax.erf(u * 0.7071067811865476))
            r.activ[i, :, w] = (u * phi).astype(BF)
            slope = phi + u * jnp.exp(-0.5 * u * u) * 0.3989422804014327
            g = dot_nt(r.cot[i], r.wdn[w, :]) * slope
            r.actlow[i, :, w] = g.astype(BF)
            r.acc[6, :, w] += fold8(g)

        tiles(F, tile)

    def norm2_part(i):
        def tile(w):
            r.own3[i, :, w] = dot_nt(r.actlow[i], r.wup[w, :]).astype(BF)

        tiles(D, tile)

    def out_part(i):
        def tile(w):
            r.own2[i, :, w] = dot(r.activ[i], r.wdn[:, w]).astype(BF)

        tiles(D, tile)

    for i in range(I):
        sum_end(1, i)
        middle_of(i)
        if i == 0:
            weight_ready(UP)
            weight_ready(DN)
        feed_forward(i)
        norm2_part(i)
        sum_start(3, i)
        if i:
            sum_mid(3, i - 1)
    sum_mid(3, I - 1)
    for i in range(I):
        out_part(i)
        sum_start(2, i)

    grads = {
        QKV: (r.gqkv, r.r1qkv, r.r2qkv, r.r3qkv, r.fqkv),
        OUT: (r.gout, r.r1out, r.r2out, r.r3out, r.fout),
        UP: (r.gup, r.r1up, r.r2up, r.r3up, r.fup),
        DN: (r.gdn, r.r1dn, r.r2dn, r.r3dn, r.fdn),
    }

    def lanes_half(name):
        return name in (QKV, UP)

    def whole_half(name, ref, half):
        n = {QKV: W, UP: F, OUT: W, DN: F}[name] // 2
        w = pl.ds(aligned(half * n, n), n)
        if name == QKV:
            return ref.at[:, :, w]
        if name == UP:
            return ref.at[:, w]
        return ref.at[w, :]

    def shard_part(name, ref, shard):
        w = pl.ds(aligned(shard * part, part), part)
        if name == QKV:
            return ref.at[:, w, :]
        if name == UP:
            return ref.at[w, :]
        return ref.at[:, w]

    def add_into(dst, a, b):
        shape = dst.shape
        planes = shape[0] if len(shape) == 3 else 1
        n = shape[-2]
        for pln in range(planes):
            pick = (lambda ref: ref.at[pln]) if len(shape) == 3 else (lambda ref: ref)
            da, aa, bb = pick(dst), pick(a), pick(b)

            def step(k, _):
                w = pl.ds(aligned(k * RB, RB), RB)
                da[w, :] = (aa[w, :].astype(F32) + bb[w, :].astype(F32)).astype(BF)
                return 0

            lax.fori_loop(0, n // RB, step, 0)

    red = {}

    def reduce1(name):
        g, r1, r2, r3, f = grads[name]
        red[name, 1] = net.remote(whole_half(name, g, 1 - core), r1, on_mate)
        go(red[name, 1])

    def reduce2(name):
        g, r1, r2, r3, f = grads[name]
        red[name, 1].wait_recv()
        add_into(r1, whole_half(name, g, core), r1)
        for ds in range(1, S):
            to = lax.rem(s + ds, S)
            red[name, 2, ds] = net.remote(shard_part(name, r1, to), r2.at[ds], (to, c, t))
            go(red[name, 2, ds])

    def reduce3(name):
        g, r1, r2, r3, f = grads[name]
        for ds in range(1, S):
            red[name, 2, ds].wait_recv()
            first = shard_part(name, r1, s) if ds == 1 else r2.at[0]
            add_into(r2.at[0], first, r2.at[ds])
        red[name, 3] = net.remote(r2.at[0], r3, on_across)
        go(red[name, 3])

    def reduce4(name):
        g, r1, r2, r3, f = grads[name]
        red[name, 3].wait_recv()
        mine = whole_half(name, f, core)
        add_into(mine, r2.at[0], r3)
        red[name, 4] = net.remote(mine, mine, on_mate)
        go(red[name, 4])

    def flat(ref, w=None):
        v = ref[...] if w is None else ref[:, :, w]
        return v.reshape(I * R, v.shape[-1])

    def grad_down():
        def tile(w):
            r.gdn[w, :] = dot_tn(flat(r.activ, w), flat(r.cot)).astype(BF)

        tiles(F, tile)

    def grad_up():
        def tile(w):
            r.gup[w, :] = dot_tn(flat(r.second, w), flat(r.actlow)).astype(BF)

        tiles(D, tile)

    def grad_out():
        r.gout[...] = dot_tn(flat(r.att), flat(r.mlow)).astype(BF)

    def grad_qkv():
        def tile(w):
            x = flat(r.first, w)
            for n in range(3):
                r.gqkv[n, w, :] = dot_tn(x, flat(r.pg.at[n])).astype(BF)

        tiles(D, tile)

    grad_down()
    reduce1(DN)
    grad_up()
    reduce1(UP)
    reduce2(DN)
    reduce2(UP)

    def middle_back(i):
        def rows(w):
            unit, inv = norm_stats(r.middle[i, w, :])
            n2 = r.tot3[i, w, :].astype(F32)
            up = r.cot[i, w, :].astype(F32)
            g = up + norm_back(n2, unit, inv, r.g2[...])
            r.mgrad[i, w, :] = g
            r.mlow[i, w, :] = g.astype(BF)
            r.acc[1] += fold8(g)
            r.acc[4] += fold8(n2 * unit)
            r.acc[5] += fold8(n2)
            r.acc[7] += fold8(up)

        blocks(rows)

    def attention_back(i):
        k, v = all_keys(i)
        q = r.q[i].astype(F32)
        grad = dot_nt(r.mlow[i], r.wout[...])
        grad = grad.astype(BF).astype(F32)

        def head(h, total):
            mine = lane_head == h
            w = pl.ds(aligned(h * R, R), R)
            gh = jnp.where(mine, grad, 0.0).astype(BF)
            r.ost[w, :] = gh
            r.qst[w, :] = jnp.where(mine, q, 0.0).astype(BF)
            wg = dot_nt(gh, v)
            p = r.wts[i, w, :].astype(F32)
            pw = p * wg
            row_dot = jnp.sum(pw, axis=-1, keepdims=True)
            ds = ((pw - p * row_dot) * scale).astype(BF)
            r.dss[w, :] = ds
            return jnp.where(mine, dot(ds, k), total)

        dq = lax.fori_loop(0, heads, head, jnp.zeros((R, W), F32))
        r.acc[0, :, 0:W] += fold8(dq)
        r.pg[0, i] = dq.astype(BF)
        dk = dot_tn(r.dss[...], r.qst[...]).astype(BF)
        dv = dot_tn(r.wts[i], r.ost[...]).astype(BF)
        for b in range(C):
            r.dkv[b, i, 0] = dk[b * R : (b + 1) * R, :]
            r.dkv[b, i, 1] = dv[b * R : (b + 1) * R, :]

    back_mate, back_far, back_across = {}, {}, {}

    def key_send(i):
        back_far[i] = net.remote(r.dkv.at[far, i], r.rxa.at[1, i], on_mate)
        back_mate[i] = net.remote(r.dkv.at[mate, i], r.rxa.at[0, i], on_mate)
        go(back_far[i])
        go(back_mate[i])

    def key_mid(i):
        back_far[i].wait_recv()
        for n in range(2):
            both = r.dkv[across, i, n].astype(F32) + r.rxa[1, i, n].astype(F32)
            r.rxa[1, i, n] = both.astype(BF)
        back_across[i] = net.remote(r.rxa.at[1, i], r.rxb.at[i], on_across)
        go(back_across[i])

    def key_end(i):
        back_mate[i].wait_recv()
        back_across[i].wait_recv()
        for n in range(2):
            both = r.dkv[c, i, n].astype(F32) + r.rxa[0, i, n].astype(F32)
            both = both + r.rxb[i, n].astype(F32)
            r.pg[1 + n, i] = both.astype(BF)
            if n == 1:
                r.acc[0, :, W : 2 * W] += fold8(both)

    def norm1_part(i):
        def tile(w):
            total = dot_nt(r.pg[0, i], r.wqkv[0, w, :])
            total = total + dot_nt(r.pg[1, i], r.wqkv[1, w, :])
            total = total + dot_nt(r.pg[2, i], r.wqkv[2, w, :])
            r.own4[i, :, w] = total.astype(BF)

        tiles(D, tile)

    for i in range(I):
        sum_end(3, i)
        middle_back(i)
        attention_back(i)
        key_send(i)
        key_mid(i)
        sum_mid(2, i)
    for i in range(I):
        key_end(i)
        norm1_part(i)
        sum_start(4, i)
        if i:
            sum_mid(4, i - 1)
    sum_mid(4, I - 1)
    grad_out()
    reduce1(OUT)
    grad_qkv()
    reduce1(QKV)
    reduce3(DN)
    reduce3(UP)
    reduce2(OUT)
    reduce2(QKV)

    puts = []

    def out_rows(i):
        def rows(w):
            x = r.middle[i, w, :] + r.tot2[i, w, :].astype(F32) + r.bdn[...]
            r.middle[i, w, :] = x

        blocks(rows)
        put = net.local(r.middle.at[i, pl.ds(0, piece)], r.out_h.at[i])
        put.start()
        puts.append(put)

    def token_rows(i):
        def rows(w):
            unit, inv = norm_stats(r.tok[i, w, :].astype(F32))
            n1 = r.tot4[i, w, :].astype(F32)
            g = r.mgrad[i, w, :] + norm_back(n1, unit, inv, r.g1[...])
            r.mgrad[i, w, :] = g
            r.acc[2] += fold8(n1 * unit)
            r.acc[3] += fold8(n1)

        blocks(rows)
        put = net.local(r.mgrad.at[i, pl.ds(0, piece)], r.gtok_h.at[i])
        put.start()
        puts.append(put)

    for i in range(I):
        sum_end(2, i)
        out_rows(i)
    reduce4(DN)
    reduce4(UP)
    reduce3(OUT)
    reduce3(QKV)
    for i in range(I):
        sum_end(4, i)
        token_rows(i)

    for k in range(8):
        r.sm[k : k + 1, :] = jnp.sum(r.acc[k], axis=0, keepdims=True)
    slot = s * C + c
    r.smx[slot] = r.sm[...]
    small = []
    for ds in range(S):
        for dc in range(C):
            if ds or dc:
                to = (lax.rem(s + ds, S), lax.rem(c + dc, C), t)
                copy = net.remote(r.sm, r.smx.at[slot], to)
                go(copy)
                small.append(copy)
    reduce4(OUT)
    reduce4(QKV)
    for copy in small:
        copy.wait_recv()

    def add_slot(n, total):
        return total + r.smx[n]

    r.smo[...] = lax.fori_loop(1, S * C, add_slot, r.smx[0])
    for name in grads:
        red[name, 4].wait_recv()
    for put in puts:
        put.wait()
    for _, copy in sent:
        copy.wait_send()

    @pl.when(edge)
    def _():
        for copy in hop0.values():
            copy.wait_send()

    @pl.when(inner)
    def _():
        for copy in hop1.values():
            copy.wait_send()
        for copy in hop2.values():
            copy.wait_send()


def call_kernel(d, ins):
    scratch = scratch_of(d)
    I, D, W, F = d.images, d.width, d.local, d.hidden
    vmem = pl.BlockSpec(memory_space=pltpu.VMEM)
    hbm = pl.BlockSpec(memory_space=pl.ANY)
    arr = jax.ShapeDtypeStruct
    outs = dict(
        out_h=arr((I, d.piece, D), F32),
        gtok_h=arr((I, d.piece, D), F32),
        fqkv=arr((3, d.part, W), BF),
        fout=arr((W, d.part), BF),
        fup=arr((d.part, F), BF),
        fdn=arr((F, d.part), BF),
        smo=arr((8, D), F32),
    )
    names = (*ins, *outs, *scratch)
    return pl.pallas_call(
        functools.partial(body_kernel, d, names),
        out_shape=tuple(outs.values()),
        in_specs=[hbm] * 6 + [vmem] * 9,
        out_specs=(hbm, hbm, vmem, vmem, vmem, vmem, vmem),
        scratch_shapes=list(scratch.values()),
        compiler_params=pltpu.CompilerParams(
            collective_id=0, has_side_effects=True, vmem_limit_bytes=67043328
        ),
        name="encoder_layer",
    )(*ins.values())


def body(mesh, tokens, pad_mask, ln1_gain, ln1_shift, w_qkv, b_qv, w_out, b_out, ln2_gain, ln2_shift, w_up, b_up, w_down, b_down, cotangent):
    d = dims_of(mesh, tokens.shape, w_out.shape, w_up.shape)
    row = lambda v: v.reshape(1, -1)
    ins = dict(
        tok_h=tokens,
        cot_h=cotangent,
        wqkv_h=w_qkv,
        wout_h=w_out,
        wup_h=w_up,
        wdn_h=w_down,
        mask=pad_mask,
        g1=row(ln1_gain),
        b1=row(ln1_shift),
        bqv=b_qv,
        bout=row(b_out),
        g2=row(ln2_gain),
        b2=row(ln2_shift),
        bup=row(b_up),
        bdn=row(b_down),
    )
    out, gtok, fqkv, fout, fup, fdn, small = call_kernel(d, ins)
    W = d.local
    return (
        out,
        gtok,
        fqkv.astype(F32),
        small[0, : 2 * W].reshape(2, W),
        fout.astype(F32),
        small[1],
        small[2],
        small[3],
        small[4],
        small[5],
        fup.astype(F32),
        small[6, : d.hidden],
        fdn.astype(F32),
        small[7],
    )


def solution(mesh):
    return jax.shard_map(
        functools.partial(body, mesh),
        mesh=mesh,
        in_specs=(
            P("shard", "ctx", None),
            P("shard", "ctx"),
            P(),
            P(),
            P(None, "shard", "tp"),
            P(None, "tp"),
            P("tp", "shard"),
            P(),
            P(),
            P(),
            P("shard", "tp"),
            P("tp"),
            P("tp", "shard"),
            P(),
            P("shard", "ctx", None),
        ),
        out_specs=(
            P("shard", "ctx", None),
            P("shard", "ctx", None),
            P(None, "shard", "tp"),
            P(None, "tp"),
            P("tp", "shard"),
            P(),
            P(),
            P(),
            P(),
            P(),
            P("shard", "tp"),
            P("tp"),
            P("tp", "shard"),
            P(),
        ),
        check_vma=False,
    )
```

```python
import functools
import math
import types

import jax
import jax.numpy as jnp
from jax import lax
from jax.experimental import pallas as pl
from jax.experimental.pallas import tpu as pltpu
from jax.sharding import PartitionSpec as P

HD = 64
BIG = 1e30
MESH = pl.DeviceIdType.MESH
BF, F32 = jnp.bfloat16, jnp.float32
RB = 32
TILE = 256


KV, Q, OUT, UP, DN = range(5)
Q0, K0, V0, OUT0, UP0, UP1, DN0, DN1 = range(8)
PIECES = (DN0, DN1, UP0, UP1, OUT0, Q0, K0, V0)
(
    LN, FW, KVP, QP, KF, AT, P1, SS, SJ, SM, SE, MO, FF, P3, P2, MB, AB, KM, KE, P4, OR, TR,
    GD, GU, GO, GQ, R2, R3, R4, SMA, SMB, FIN,
) = range(32)
CUTS = ((0, 80), (80, 72))
ORDER = (
    (LN, 2), (LN, 0), (LN, 1), (FW, KV), (KVP, 0), (FW, Q), (QP, 1), (QP, 2), (KVP, 1), (KVP, 2),
    (KF, 0), (QP, 0), (FW, OUT), (AT, 0), (P1, 0), (SS, 1, 0), (KF, 1), (AT, 1), (KF, 2), (P1, 1),
    (SM, 1, 0, 0), (SS, 1, 1), (AT, 2), (SM, 1, 0, 1), (SE, 1, 0, 0), (SM, 1, 1, 0), (FW, UP),
    (SE, 1, 0, 1), (P1, 2), (SM, 1, 1, 1), (SS, 1, 2), (FW, DN), (MO, 0), (SE, 1, 1, 0),
    (SM, 1, 2, 0), (FF, 0), (P3, 0), (SE, 1, 1, 1), (SM, 1, 2, 1), (SS, 3, 0), (MO, 1), (FF, 1),
    (SE, 1, 2, 0), (P3, 1), (SS, 3, 1), (P2, 0), (SE, 1, 2, 1), (MO, 2), (SM, 3, 0, 0), (FF, 2),
    (P3, 2), (SM, 3, 0, 1), (SS, 3, 2), (GD,), (SJ, 2, 0, 1), (SE, 3, 0, 0), (P2, 1), (SM, 3, 1, 0),
    (SJ, 2, 1, 0), (GU,), (SE, 3, 0, 1), (SM, 3, 1, 1), (R2, DN0), (P2, 2), (MB, 0), (SE, 3, 1, 0),
    (SM, 3, 2, 0), (AB, 0), (SM, 3, 2, 1), (SE, 3, 1, 1), (SJ, 2, 2, 1), (KM, 0), (R3, DN0),
    (R2, DN1), (SJ, 2, 1, 1), (MB, 1), (SJ, 2, 0, 0), (SM, 2, 0, 1), (SE, 3, 2, 0), (AB, 1),
    (SE, 3, 2, 1), (R2, UP1), (SM, 2, 1, 0), (KE, 0), (R2, UP0), (P4, 0), (KM, 1), (SE, 2, 0, 1),
    (SM, 2, 2, 1), (MB, 2), (SS, 4, 0), (R3, DN1), (SM, 2, 1, 1), (SE, 2, 1, 0), (AB, 2),
    (SE, 2, 2, 1), (SM, 2, 0, 0), (KE, 1), (P4, 1), (SS, 4, 1), (KM, 2), (GO,), (SM, 4, 0, 0),
    (SE, 2, 1, 1), (GQ, 0), (R3, UP0), (OR, 1), (R4, DN1), (R2, Q0), (SM, 4, 0, 1), (R3, UP1),
    (SE, 2, 0, 0), (KE, 2), (P4, 2), (SM, 4, 1, 0), (SS, 4, 2), (GQ, 2), (SE, 4, 0, 0), (OR, 0),
    (R2, OUT0), (GQ, 1), (SJ, 2, 2, 0), (R3, Q0), (SE, 4, 0, 1), (R2, K0), (SM, 4, 1, 1), (R4, UP0),
    (TR, 0), (SE, 4, 1, 0), (R2, V0), (SM, 4, 2, 0), (SE, 4, 1, 1), (R3, K0), (SM, 4, 2, 1),
    (R4, Q0), (SMA,), (TR, 1), (R3, OUT0), (SE, 4, 2, 0), (R3, V0), (R4, DN0), (SM, 2, 2, 0),
    (SE, 4, 2, 1), (SE, 2, 2, 0), (R4, UP1), (R4, OUT0), (TR, 2), (SMB,), (R4, K0), (R4, V0),
    (OR, 2), (FIN,),
)


def dot(a, b):
    return lax.dot_general(a, b, (((1,), (0,)), ((), ())), preferred_element_type=F32)


def dot_nt(a, b):
    return lax.dot_general(a, b, (((1,), (1,)), ((), ())), preferred_element_type=F32)


def dot_tn(a, b):
    return lax.dot_general(a, b, (((0,), (0,)), ((), ())), preferred_element_type=F32)


def norm_stats(x):
    centred = x - jnp.mean(x, axis=-1, keepdims=True)
    inv = lax.rsqrt(jnp.mean(centred * centred, axis=-1, keepdims=True) + 1e-06)
    return centred * inv, inv


def norm_back(upstream, unit, inv, gain):
    scaled = upstream * gain
    centre = jnp.mean(scaled, axis=-1, keepdims=True)
    along = jnp.mean(scaled * unit, axis=-1, keepdims=True)
    return inv * (scaled - centre - unit * along)


def fold8(x):
    return jnp.sum(x.reshape(x.shape[0] // 8, 8, x.shape[1]), axis=0)


def aligned(i, m):
    return pl.multiple_of(i, m)


def span(i, n):
    return pl.ds(aligned(i * n, n), n)


class Dims:
    pass


def dims_of(mesh, tokens, w_out, w_up):
    d = Dims()
    d.S, d.C, d.T = (mesh.shape[a] for a in ("shard", "ctx", "tp"))
    assert d.C == 4 and d.T == 4
    d.images, d.piece, d.width = tokens
    d.rows = -(-d.piece // RB) * RB
    d.part = d.width // d.S
    d.local = w_out[0]
    d.hidden = w_up[1]
    d.heads = d.local // HD
    d.keys = d.C * d.rows
    assert d.rows > d.piece
    return d


def scratch_of(d):
    I, R, D, W, F, S, C = d.images, d.rows, d.width, d.local, d.hidden, d.S, d.C
    bf = lambda *shape: pltpu.VMEM(shape, BF)
    f32 = lambda *shape: pltpu.VMEM(shape, F32)
    scratch = dict(
        tok=bf(I, R, D),
        cot=bf(I, R, D),
        maskw=f32(8, TILE),
        first=bf(I, R, D),
        wqkv=bf(3, D, W),
        wout=bf(W, D),
        wup=bf(D, F),
        wdn=bf(F, D),
        q=bf(I, R, W),
        kv=bf(C, I, 2, R, W),
        wts=bf(I, d.heads * R, d.keys),
        att=bf(I, R, W),
        middle=f32(I, R, D),
        second=bf(I, R, D),
        activ=bf(I, R, F),
        actlow=bf(I, R, F),
        mgrad=f32(I, R, D),
        mlow=bf(I, R, D),
        dss=bf(d.heads * R, d.keys),
        qst=bf(d.heads * R, W),
        ost=bf(d.heads * R, W),
        dkv=bf(C, I, 2, R, W),
        rxa=bf(2, I, 2, R, W),
        rxb=bf(I, 2, R, W),
        pg=bf(3, I, R, W),
        acc=f32(8, 8, D),
        sm=f32(8, D),
        smx=f32(S * C, 8, D),
        gqkv=bf(3, D, W),
        gout=bf(W, D),
        gup=bf(D, F),
        gdn=bf(F, D),
        r1q=bf(3, D, W // 2),
        r1o=bf(W // 2, D),
        r1u=bf(2, D, F // 4),
        r1d=bf(2, F // 4, D),
        r2q=bf(3, S, D // S, W // 2),
        r2o=bf(S, W // 2, D // S),
        r2u=bf(2, S, D // S, F // 4),
        r2d=bf(2, S, F // 4, D // S),
        r3q=bf(3, D // S, W // 2),
        r3o=bf(W // 2, D // S),
        r3u=bf(2, D // S, F // 4),
        r3d=bf(2, F // 4, D // S),
        fqkv=bf(3, D // S, W),
        fout=bf(W, D // S),
        fup=bf(D // S, F),
        fdn=bf(F, D // S),
        mask=pltpu.VMEM((I, d.piece), jnp.int32),
        g1=f32(1, D),
        b1=f32(1, D),
        bqv=f32(2, W),
        bout=f32(1, D),
        g2=f32(1, D),
        b2=f32(1, D),
        bup=f32(1, F),
        bdn=f32(1, D),
        smt=f32(8, D // 4),
        smtx=f32(S * C, 8, D // 4),
    )
    full = lambda: bf(I, R, D)
    scratch.update(own1=full(), own2=full(), own3=full(), own4=full())
    scratch.update(tot1=full(), tot2=full(), tot3=full(), tot4=full())
    scratch.update(in01=full(), in02=full(), in03=full())
    scratch.update(in11=full(), in12=full(), in13=full())
    scratch["ssem"] = pltpu.SemaphoreType.DMA((MAX_COPIES * S // 2,))
    scratch["rsem"] = pltpu.SemaphoreType.DMA((MAX_COPIES * S // 2,))
    scratch["lsem"] = pltpu.SemaphoreType.DMA((64,))
    return scratch


MAX_COPIES = 320


class Net:
    def __init__(self, ssem, rsem, lsem):
        self.ssem, self.rsem, self.lsem = ssem, rsem, lsem
        self.n = self.m = 0
        self.sent = []
        self.stored = []

    def remote(self, src, dst, device):
        i, self.n = self.n, self.n + 1
        return pltpu.make_async_remote_copy(
            src_ref=src,
            dst_ref=dst,
            send_sem=self.ssem.at[i],
            recv_sem=self.rsem.at[i],
            device_id=device,
            device_id_type=MESH,
        )

    def local(self, src, dst):
        i, self.m = self.m, self.m + 1
        return pltpu.make_async_copy(src, dst, self.lsem.at[i])


def body_kernel(d, names, *refs):
    r = types.SimpleNamespace(**dict(zip(names, refs)))
    I, R, D, W, F, S, C = d.images, d.rows, d.width, d.local, d.hidden, d.S, d.C
    piece, part, heads, keys = d.piece, d.part, d.heads, d.keys
    s, c, t = lax.axis_index("shard"), lax.axis_index("ctx"), lax.axis_index("tp")
    core = lax.rem(c, 2)
    mate = c + 1 - 2 * core
    across = lax.rem(c + 2, 4)
    far = lax.rem(mate + 2, 4)
    tmate = t + 1 - 2 * lax.rem(t, 2)
    tpeer = 3 - t
    inner = lax.rem(t + 1, 4) >= 2
    edge = lax.rem(t + 1, 4) < 2
    on_mate, on_across = (s, mate, t), (s, across, t)
    net = Net(r.ssem, r.rsem, r.lsem)
    sent = net.sent

    def go(copy):
        copy.start()
        sent.append((None, copy))

    tail = piece // 16 * 16
    for ref in (r.tot1, r.tot2, r.tot3, r.tot4, r.in01, r.in02, r.in03, r.in11, r.in12, r.in13):
        for i in range(I):
            ref[i, tail:R, :] = jnp.zeros((R - tail, D), BF)
    for i in range(I):
        for n in range(2):
            r.rxb[i, n, tail:R, :] = jnp.zeros((R - tail, W), BF)
            for b in range(2):
                r.rxa[b, i, n, tail:R, :] = jnp.zeros((R - tail, W), BF)

    barrier = pltpu.get_barrier_semaphore()
    pl.semaphore_signal(barrier, inc=1, device_id=(s, c, tmate), device_id_type=MESH)
    for ds in range(S):
        for dc in range(C):
            if ds or dc:
                where = (lax.rem(s + ds, S), lax.rem(c + dc, C), t)
                pl.semaphore_signal(barrier, inc=1, device_id=where, device_id_type=MESH)

    @pl.when(inner)
    def _():
        pl.semaphore_signal(barrier, inc=1, device_id=(s, c, tpeer), device_id_type=MESH)

    loads = {}
    for i in range(I):
        loads[LN, i] = net.local(r.tok_h.at[i], r.tok.at[i, pl.ds(0, piece)])
    vectors = [
        net.local(a, b)
        for a, b in (
            (r.mask_h, r.mask),
            (r.g1_h, r.g1),
            (r.b1_h, r.b1),
            (r.bqv_h, r.bqv),
            (r.bout_h, r.bout),
            (r.g2_h, r.g2),
            (r.b2_h, r.b2),
            (r.bup_h, r.bup),
            (r.bdn_h, r.bdn),
        )
    ]
    rows_s = span(s, part)
    loads[KV] = net.local(r.wqkv_h.at[pl.ds(1, 2)], r.wqkv.at[pl.ds(1, 2), rows_s])
    loads[Q] = net.local(r.wqkv_h.at[pl.ds(0, 1)], r.wqkv.at[pl.ds(0, 1), rows_s])
    loads[OUT] = net.local(r.wout_h, r.wout.at[:, rows_s])
    loads[UP] = net.local(r.wup_h, r.wup.at[rows_s])
    loads[DN] = net.local(r.wdn_h, r.wdn.at[:, rows_s])
    for i in range(I):
        loads[FF, i] = net.local(r.cot_h.at[i], r.cot.at[i, pl.ds(0, piece)])
    for copy in (*loads.values(), *vectors):
        copy.start()

    @pl.when(inner)
    def _():
        pl.semaphore_wait(barrier, S * C + 1)

    @pl.when(edge)
    def _():
        pl.semaphore_wait(barrier, S * C)

    def half_of(name, ref, shard, half):
        rows = pl.ds(aligned(shard * part, part), part)
        if name in (KV, Q):
            planes = pl.ds(1, 2) if name == KV else pl.ds(0, 1)
            return ref.at[planes, rows, pl.ds(aligned(half * (W // 2), W // 2), W // 2)]
        if name == OUT:
            return ref.at[pl.ds(aligned(half * (W // 2), W // 2), W // 2), rows]
        if name == UP:
            return ref.at[rows, pl.ds(aligned(half * (F // 2), F // 2), F // 2)]
        return ref.at[pl.ds(aligned(half * (F // 2), F // 2), F // 2), rows]

    def own_half(name, ref, half):
        if name in (KV, Q):
            planes = pl.ds(1, 2) if name == KV else pl.ds(0, 1)
            return ref.at[planes, :, pl.ds(aligned(half * (W // 2), W // 2), W // 2)]
        if name == OUT:
            return ref.at[pl.ds(aligned(half * (W // 2), W // 2), W // 2), :]
        if name == UP:
            return ref.at[:, pl.ds(aligned(half * (F // 2), F // 2), F // 2)]
        return ref.at[pl.ds(aligned(half * (F // 2), F // 2), F // 2), :]

    weights = {
        KV: (r.wqkv_h, r.wqkv),
        Q: (r.wqkv_h, r.wqkv),
        OUT: (r.wout_h, r.wout),
        UP: (r.wup_h, r.wup),
        DN: (r.wdn_h, r.wdn),
    }
    gather, spread = {}, {}
    for name, (source, full) in weights.items():
        for ds in range(1, S):
            to = (lax.rem(s + ds, S), c, t)
            copy = net.remote(
                own_half(name, source, core), half_of(name, full, s, core), to
            )
            go(copy)
            gather[name, ds] = copy
            owner = lax.rem(s + S - ds, S)
            held = half_of(name, full, owner, core)
            spread[name, ds] = net.remote(held, held, on_mate)

    def pass_on(name):
        for ds in range(1, S):
            gather[name, ds].wait_recv()
            go(spread[name, ds])

    arrived = set()

    def weight_ready(name):
        if name in arrived:
            return
        arrived.add(name)
        loads[name].wait()
        for ds in range(1, S):
            spread[name, ds].wait_recv()

    def clear_tail(ref, i):
        if tail < R:
            old = ref[i, pl.ds(tail, R - tail), :].astype(F32)
            row = lax.broadcasted_iota(jnp.int32, old.shape, 0)
            ref[i, pl.ds(tail, R - tail), :] = jnp.where(row < piece - tail, old, 0.0).astype(BF)

    def blocks(fn):
        n = R // 2

        def step(b, _):
            fn(span(b, n))
            return 0

        lax.fori_loop(0, 2, step, 0)

    def tiles(n, fn):
        def step(b, _):
            fn(pl.ds(aligned(b * TILE, TILE), TILE))
            return 0

        lax.fori_loop(0, n // TILE, step, 0)

    r.acc[...] = jnp.zeros_like(r.acc)
    r.sm[...] = jnp.zeros_like(r.sm)
    r.maskw[...] = jnp.zeros_like(r.maskw)
    for copy in vectors:
        copy.wait()
    r.maskw[0:I, 0:piece] = (r.mask[...] > 0).astype(F32)

    def first_norm(i):
        loads[LN, i].wait()
        clear_tail(r.tok, i)

        def rows(w):
            unit, _ = norm_stats(r.tok[i, w, :].astype(F32))
            r.first[i, w, :] = (unit * r.g1[...] + r.b1[...]).astype(BF)

        blocks(rows)

    kv_mate, kv_across, kv_far = {}, {}, {}
    row_w = lax.broadcasted_iota(jnp.int32, (R, W), 0)

    def keys_values(i):
        weight_ready(KV)
        x = r.first[i]
        key = dot(x, r.wqkv[1])
        flags = jnp.broadcast_to(r.maskw[i : i + 1, :], (R, W))
        r.kv[c, i, 0] = jnp.where(row_w == piece, flags, key).astype(BF)
        r.kv[c, i, 1] = (dot(x, r.wqkv[2]) + r.bqv[1:2, :]).astype(BF)
        mine = r.kv.at[c, i]
        kv_across[i] = net.remote(mine, mine, on_across)
        kv_mate[i] = net.remote(mine, mine, on_mate)
        theirs = r.kv.at[across, i]
        kv_far[i] = net.remote(theirs, theirs, on_mate)
        go(kv_across[i])
        go(kv_mate[i])

    def queries(i):
        weight_ready(Q)
        r.q[i] = (dot(r.first[i], r.wqkv[0]) + r.bqv[0:1, :]).astype(BF)

    def key_forward(i):
        kv_across[i].wait_recv()
        go(kv_far[i])

    lane_head = lax.broadcasted_iota(jnp.int32, (R, W), 1) // HD
    scale = 1.0 / math.sqrt(HD)

    def all_keys(i):
        k = jnp.concatenate([r.kv[b, i, 0] for b in range(C)], axis=0)
        v = jnp.concatenate([r.kv[b, i, 1] for b in range(C)], axis=0)
        return k, v

    def key_bias(i):
        row = lax.broadcasted_iota(jnp.int32, (R, W), 0)
        lane = lax.broadcasted_iota(jnp.int32, (R, W), 1)
        lane1 = lax.broadcasted_iota(jnp.int32, (R, 128), 1)
        columns = []
        for b in range(C):
            low = r.kv[b, i, 0, pl.ds(tail, 16), :].astype(F32)
            flags = low[piece - tail : piece - tail + 1, :]
            flag = jnp.sum(jnp.where(row == lane, flags, 0.0), axis=1, keepdims=True)
            columns.append(jnp.where(lane1 == 0, (flag - 1.0) * BIG, 0.0).astype(BF))
        pick = lax.broadcasted_iota(jnp.int32, (16, 128), 1)
        pick = jnp.where(pick == 0, 1.0, 0.0).astype(BF)
        return dot_nt(pick, jnp.concatenate(columns, axis=0))[0:1, :]

    def attention(i):
        kv_far[i].wait_recv()
        kv_mate[i].wait_recv()
        k, v = all_keys(i)
        bias = key_bias(i)
        q = r.q[i].astype(F32)

        def head(h, total):
            mine = lane_head == h
            qh = jnp.where(mine, q, 0.0).astype(BF)
            scores = dot_nt(qh, k) * scale + bias
            top = jnp.max(scores, axis=-1, keepdims=True)
            e = jnp.exp(scores - top)
            w = (e * (1.0 / jnp.sum(e, axis=-1, keepdims=True))).astype(BF)
            r.wts[i, pl.ds(aligned(h * R, R), R), :] = w
            return jnp.where(mine, dot(w, v), total)

        total = lax.fori_loop(0, heads, head, jnp.zeros((R, W), F32))
        r.att[i] = total.astype(BF)

    hop0, hop1, hop2 = {}, {}, {}

    def sum_plan(k, i):
        own = (r.own1, r.own2, r.own3, r.own4)[k - 1]
        tot = (r.tot1, r.tot2, r.tot3, r.tot4)[k - 1]
        in0 = (r.in01, r.in02, r.in03, r.in01)[k - 1]
        in1 = (r.in11, r.in12, r.in13, r.in11)[k - 1]
        for j, (first, n) in enumerate(CUTS):
            w = pl.ds(first, n)
            hop0[k, i, j] = net.remote(own.at[i, w], in0.at[i, w], (s, c, tmate))
            hop1[k, i, j] = net.remote(own.at[i, w], in1.at[i, w], (s, c, tpeer))
            hop2[k, i, j] = net.remote(tot.at[i, w], tot.at[i, w], (s, c, tmate))
        return own, tot, in0, in1

    sums = {(k, i): sum_plan(k, i) for k in range(1, 5) for i in range(I)}

    def add_rows(dst, a, b, i, j):
        first, n = CUTS[j]

        def step(m, _):
            w = pl.ds(aligned(first + m * 16, 16), 16)
            dst[i, w, :] = (a[i, w, :].astype(F32) + b[i, w, :].astype(F32)).astype(BF)
            return 0

        lax.fori_loop(0, -(-n // 16), step, 0)

    def sum_block(k, i, j):
        @pl.when(edge)
        def _():
            hop0[k, i, j].start()

    def sum_start(k, i):
        @pl.when(edge)
        def _():
            for j in range(len(CUTS)):
                hop0[k, i, j].start()

    def sum_mid(k, i, j):
        own, tot, in0, in1 = sums[k, i]

        @pl.when(inner)
        def _():
            hop0[k, i, j].wait_recv()
            add_rows(own, own, in0, i, j)
            hop1[k, i, j].start()

    def sum_end(k, i, j):
        own, tot, in0, in1 = sums[k, i]

        @pl.when(inner)
        def _():
            hop1[k, i, j].wait_recv()
            add_rows(tot, own, in1, i, j)
            hop2[k, i, j].start()

    def sum_got(k, i):
        @pl.when(edge)
        def _():
            for j in range(len(CUTS)):
                hop2[k, i, j].wait_recv()

    def attn_part(i):
        weight_ready(OUT)

        def tile(w):
            r.own1[i, :, w] = dot(r.att[i], r.wout[:, w]).astype(BF)

        tiles(D, tile)

    def middle_of(i):
        sum_got(1, i)

        def rows(w):
            x = r.tok[i, w, :].astype(F32) + r.tot1[i, w, :].astype(F32) + r.bout[...]
            r.middle[i, w, :] = x
            unit, _ = norm_stats(x)
            r.second[i, w, :] = (unit * r.g2[...] + r.b2[...]).astype(BF)

        blocks(rows)

    def feed_forward(i):
        weight_ready(UP)
        weight_ready(DN)
        loads[FF, i].wait()
        clear_tail(r.cot, i)

        def tile(w):
            u = dot(r.second[i], r.wup[:, w]) + r.bup[:, w]
            phi = 0.5 * (1.0 + lax.erf(u * 0.7071067811865476))
            r.activ[i, :, w] = (u * phi).astype(BF)
            slope = phi + u * jnp.exp(-0.5 * u * u) * 0.3989422804014327
            g = dot_nt(r.cot[i], r.wdn[w, :]) * slope
            r.actlow[i, :, w] = g.astype(BF)
            r.acc[6, :, w] += fold8(g)

        tiles(F, tile)

    def norm2_part(i):
        def tile(w):
            r.own3[i, :, w] = dot_nt(r.actlow[i], r.wup[w, :]).astype(BF)

        tiles(D, tile)

    def out_part(i):
        def tile(w):
            r.own2[i, :, w] = dot(r.activ[i], r.wdn[:, w]).astype(BF)

        tiles(D, tile)

    tall = (Q0, K0, V0, UP0, UP1)

    def half_view(piece_id, half, planes, wo, up, dn):
        if piece_id in (Q0, K0, V0):
            return planes.at[piece_id, :, span(half, W // 2)]
        if piece_id == OUT0:
            return wo.at[span(half, W // 2), :]
        n = F // 4
        if piece_id in (UP0, UP1):
            return up.at[:, pl.ds(aligned(half * 2 * n + (piece_id - UP0) * n, n), n)]
        return dn.at[pl.ds(aligned(half * 2 * n + (piece_id - DN0) * n, n), n), :]

    def grad_half(p, half):
        return half_view(p, half, r.gqkv, r.gout, r.gup, r.gdn)

    def final_half(p, half):
        return half_view(p, half, r.fqkv, r.fout, r.fup, r.fdn)

    def slot_of(p, q, o, u, d_):
        if p in (Q0, K0, V0):
            return q.at[p]
        if p == OUT0:
            return o
        return u.at[p - UP0] if p in (UP0, UP1) else d_.at[p - DN0]

    def shard_part(p, ref, shard):
        w = span(shard, part)
        return ref.at[w, :] if p in tall else ref.at[:, w]

    def add_into(dst, a, b):
        def step(k, _):
            w = span(k, RB)
            dst[w, :] = (a[w, :].astype(F32) + b[w, :].astype(F32)).astype(BF)
            return 0

        lax.fori_loop(0, dst.shape[0] // RB, step, 0)

    red = {}

    def reduce1(p):
        red[p, 1] = net.remote(
            grad_half(p, 1 - core), slot_of(p, r.r1q, r.r1o, r.r1u, r.r1d), on_mate
        )
        go(red[p, 1])

    def reduce2(p):
        r1, r2 = slot_of(p, r.r1q, r.r1o, r.r1u, r.r1d), slot_of(p, r.r2q, r.r2o, r.r2u, r.r2d)
        red[p, 1].wait_recv()
        add_into(r1, grad_half(p, core), r1)
        for ds in range(1, S):
            to = lax.rem(s + ds, S)
            red[p, 2, ds] = net.remote(shard_part(p, r1, to), r2.at[ds], (to, c, t))
            go(red[p, 2, ds])

    def reduce3(p):
        r1, r2 = slot_of(p, r.r1q, r.r1o, r.r1u, r.r1d), slot_of(p, r.r2q, r.r2o, r.r2u, r.r2d)
        for ds in range(1, S):
            red[p, 2, ds].wait_recv()
            mine = shard_part(p, r1, s) if ds == 1 else r2.at[0]
            add_into(r2.at[0], mine, r2.at[ds])
        red[p, 3] = net.remote(
            r2.at[0], slot_of(p, r.r3q, r.r3o, r.r3u, r.r3d), on_across
        )
        go(red[p, 3])

    def reduce4(p):
        r2 = slot_of(p, r.r2q, r.r2o, r.r2u, r.r2d)
        red[p, 3].wait_recv()
        mine = final_half(p, core)
        add_into(mine, r2.at[0], slot_of(p, r.r3q, r.r3o, r.r3u, r.r3d))
        red[p, 4] = net.remote(mine, mine, on_mate)
        go(red[p, 4])

    def flat(ref, w=None):
        v = ref[...] if w is None else ref[:, :, w]
        return v.reshape(I * R, v.shape[-1])

    def grad_down():
        def tile(w):
            r.gdn[w, :] = dot_tn(flat(r.activ, w), flat(r.cot)).astype(BF)

        tiles(F, tile)
        reduce1(DN0)
        reduce1(DN1)

    def grad_up():
        def tile(w):
            r.gup[w, :] = dot_tn(flat(r.second, w), flat(r.actlow)).astype(BF)

        tiles(D, tile)
        reduce1(UP0)
        reduce1(UP1)

    def grad_out():
        r.gout[...] = dot_tn(flat(r.att), flat(r.mlow)).astype(BF)
        reduce1(OUT0)

    def grad_proj(n):
        def tile(w):
            r.gqkv[n, w, :] = dot_tn(flat(r.first, w), flat(r.pg.at[n])).astype(BF)

        tiles(D, tile)
        reduce1(Q0 + n)

    def middle_back(i):
        sum_got(3, i)

        def rows(w):
            unit, inv = norm_stats(r.middle[i, w, :])
            n2 = r.tot3[i, w, :].astype(F32)
            up = r.cot[i, w, :].astype(F32)
            g = up + norm_back(n2, unit, inv, r.g2[...])
            r.mgrad[i, w, :] = g
            r.mlow[i, w, :] = g.astype(BF)
            r.acc[1] += fold8(g)
            r.acc[4] += fold8(n2 * unit)
            r.acc[5] += fold8(n2)
            r.acc[7] += fold8(up)

        blocks(rows)

    def attention_back(i):
        k, v = all_keys(i)
        q = r.q[i].astype(F32)
        grad = dot_nt(r.mlow[i], r.wout[...])
        grad = grad.astype(BF).astype(F32)

        def head(h, total):
            mine = lane_head == h
            w = pl.ds(aligned(h * R, R), R)
            gh = jnp.where(mine, grad, 0.0).astype(BF)
            r.ost[w, :] = gh
            r.qst[w, :] = jnp.where(mine, q, 0.0).astype(BF)
            wg = dot_nt(gh, v)
            p = r.wts[i, w, :].astype(F32)
            pw = p * wg
            row_dot = jnp.sum(pw, axis=-1, keepdims=True)
            ds = ((pw - p * row_dot) * scale).astype(BF)
            r.dss[w, :] = ds
            return jnp.where(mine, dot(ds, k), total)

        dq = lax.fori_loop(0, heads, head, jnp.zeros((R, W), F32))
        r.acc[0, :, 0:W] += fold8(dq)
        r.pg[0, i] = dq.astype(BF)
        dk = dot_tn(r.dss[...], r.qst[...]).astype(BF)
        dv = dot_tn(r.wts[i], r.ost[...]).astype(BF)
        for b in range(C):
            r.dkv[b, i, 0] = dk[b * R : (b + 1) * R, :]
            r.dkv[b, i, 1] = dv[b * R : (b + 1) * R, :]
        key_send(i)

    back_mate, back_far, back_across = {}, {}, {}
    real = pl.ds(0, piece)

    def key_send(i):
        back_far[i] = net.remote(r.dkv.at[far, i, :, real], r.rxa.at[1, i, :, real], on_mate)
        back_mate[i] = net.remote(r.dkv.at[mate, i, :, real], r.rxa.at[0, i, :, real], on_mate)
        go(back_far[i])
        go(back_mate[i])

    def key_mid(i):
        back_far[i].wait_recv()
        for n in range(2):
            both = r.dkv[across, i, n].astype(F32) + r.rxa[1, i, n].astype(F32)
            r.rxa[1, i, n] = both.astype(BF)
        back_across[i] = net.remote(r.rxa.at[1, i, :, real], r.rxb.at[i, :, real], on_across)
        go(back_across[i])

    def key_end(i):
        back_mate[i].wait_recv()
        back_across[i].wait_recv()
        for n in range(2):
            both = r.dkv[c, i, n].astype(F32) + r.rxa[0, i, n].astype(F32)
            both = both + r.rxb[i, n].astype(F32)
            r.pg[1 + n, i] = both.astype(BF)
            if n == 1:
                r.acc[0, :, W : 2 * W] += fold8(both)

    def norm1_part(i):
        def tile(w):
            total = dot_nt(r.pg[0, i], r.wqkv[0, w, :])
            total = total + dot_nt(r.pg[1, i], r.wqkv[1, w, :])
            total = total + dot_nt(r.pg[2, i], r.wqkv[2, w, :])
            r.own4[i, :, w] = total.astype(BF)

        tiles(D, tile)

    puts = []

    def out_rows(i):
        sum_got(2, i)

        def rows(w):
            x = r.middle[i, w, :] + r.tot2[i, w, :].astype(F32) + r.bdn[...]
            r.middle[i, w, :] = x

        blocks(rows)
        put = net.local(r.middle.at[i, pl.ds(0, piece)], r.out_h.at[i])
        put.start()
        puts.append(put)

    def token_rows(i):
        sum_got(4, i)

        def rows(w):
            unit, inv = norm_stats(r.tok[i, w, :].astype(F32))
            n1 = r.tot4[i, w, :].astype(F32)
            g = r.mgrad[i, w, :] + norm_back(n1, unit, inv, r.g1[...])
            r.mgrad[i, w, :] = g
            r.acc[2] += fold8(n1 * unit)
            r.acc[3] += fold8(n1)

        blocks(rows)
        put = net.local(r.mgrad.at[i, pl.ds(0, piece)], r.gtok_h.at[i])
        put.start()
        puts.append(put)

    slot = s * C + c
    small = []

    def spread_small(mine, slots):
        slots[slot] = mine[...]
        for ds in range(S):
            for dc in range(C):
                if ds or dc:
                    to = (lax.rem(s + ds, S), lax.rem(c + dc, C), t)
                    copy = net.remote(mine, slots.at[slot], to)
                    go(copy)
                    small.append(copy)

    def small_early():
        for k in (0, 1, 4, 5, 6, 7):
            r.sm[k : k + 1, :] = jnp.sum(r.acc[k], axis=0, keepdims=True)
        spread_small(r.sm, r.smx)

    def small_late():
        n = D // 4
        for k in range(2):
            total = jnp.sum(r.acc[2 + k], axis=0, keepdims=True)
            for q in range(4):
                r.smt[4 * k + q : 4 * k + q + 1, :] = total[:, q * n : (q + 1) * n]
        spread_small(r.smt, r.smtx)

    def finish():
        for full, home, pieces in (
            (r.fdn, r.fdn_h, (DN0, DN1)),
            (r.fup, r.fup_h, (UP0, UP1)),
            (r.fout, r.fout_h, (OUT0,)),
            (r.fqkv, r.fqkv_h, (Q0, K0, V0)),
        ):
            for p in pieces:
                red[p, 4].wait_recv()
            put = net.local(full, home)
            put.start()
            puts.append(put)
        for copy in small:
            copy.wait_recv()
        r.smo[...] = lax.fori_loop(1, S * C, lambda n, x: x + r.smx[n], r.smx[0])
        r.smto[...] = lax.fori_loop(1, S * C, lambda n, x: x + r.smtx[n], r.smtx[0])
        for put in puts:
            put.wait()
        for _, copy in sent:
            copy.wait_send()

        @pl.when(edge)
        def _():
            for copy in hop0.values():
                copy.wait_send()

        @pl.when(inner)
        def _():
            for copy in (*hop1.values(), *hop2.values()):
                copy.wait_send()

    steps = {
        LN: first_norm, FW: pass_on, KVP: keys_values, QP: queries, KF: key_forward,
        AT: attention, P1: attn_part, SS: sum_start, SJ: sum_block, SM: sum_mid, SE: sum_end,
        MO: middle_of, FF: feed_forward, P3: norm2_part, P2: out_part, MB: middle_back,
        AB: attention_back, KM: key_mid, KE: key_end, P4: norm1_part, OR: out_rows,
        TR: token_rows, GD: grad_down, GU: grad_up, GO: grad_out, GQ: grad_proj, R2: reduce2,
        R3: reduce3, R4: reduce4, SMA: small_early, SMB: small_late, FIN: finish,
    }
    for step in ORDER:
        steps[step[0]](*step[1:])


def last_kernel(d, names, *refs):
    r = types.SimpleNamespace(**dict(zip(names, refs)))
    pairs = (
        (r.fdn_i, r.fdn_v, r.fdn_w, r.fdn_o),
        (r.fup_i, r.fup_v, r.fup_w, r.fup_o),
        (r.fqkv_i, r.fqkv_v, r.fqkv_w, r.fqkv_o),
        (r.fout_i, r.fout_v, r.fout_w, r.fout_o),
        (r.out_i, None, r.out_w, r.out_o),
        (r.gtok_i, None, r.gtok_w, r.gtok_o),
    )
    takes = []
    for n, (src, low, wide, dst) in enumerate(pairs):
        takes.append(pltpu.make_async_copy(src, wide if low is None else low, r.sem.at[2 * n]))
        takes[-1].start()
    W, D, F = d.local, d.width, d.hidden
    r.bqv_o[0:1, :] = r.small[0:1, 0:W]
    r.bqv_o[1:2, :] = r.small[0:1, W : 2 * W]
    r.bout_o[...] = r.small[1:2, :]
    r.g2_o[...] = r.small[4:5, :]
    r.b2_o[...] = r.small[5:6, :]
    r.bup_o[...] = r.small[6:7, 0:F]
    r.bdn_o[...] = r.small[7:8, :]
    n4 = D // 4
    for q in range(4):
        w = pl.ds(q * n4, n4)
        r.g1_o[:, w] = r.late[q : q + 1, :]
        r.b1_o[:, w] = r.late[4 + q : 5 + q, :]
    puts = []
    for n, (src, low, wide, dst) in enumerate(pairs):
        takes[n].wait()
        if low is not None:
            planes = [(low.at[k], wide.at[k]) for k in range(3)] if len(low.shape) == 3 else [(low, wide)]
            for a, b in planes:
                step_rows = 64 if a.shape[0] % 64 == 0 else RB

                def step(k, _, a=a, b=b, m=step_rows):
                    w = span(k, m)
                    b[w, :] = a[w, :].astype(F32)
                    return 0

                lax.fori_loop(0, a.shape[0] // step_rows, step, 0)
        puts.append(pltpu.make_async_copy(wide, dst, r.sem.at[2 * n + 1]))
        puts[-1].start()
    for put in puts:
        put.wait()


def call_last(d, out, gtok, fqkv, fout, fup, fdn, small, late):
    I, D, W, F = d.images, d.width, d.local, d.hidden
    arr = jax.ShapeDtypeStruct
    ins = dict(out_i=out, gtok_i=gtok, fqkv_i=fqkv, fout_i=fout, fup_i=fup, fdn_i=fdn)
    ins.update(small=small, late=late)
    outs = dict(out_o=arr(out.shape, F32), gtok_o=arr(gtok.shape, F32))
    outs.update(fqkv_o=arr(fqkv.shape, F32), fout_o=arr(fout.shape, F32))
    outs.update(fup_o=arr(fup.shape, F32), fdn_o=arr(fdn.shape, F32))
    outs.update(bqv_o=arr((2, W), F32), bout_o=arr((1, D), F32), g1_o=arr((1, D), F32))
    outs.update(b1_o=arr((1, D), F32), g2_o=arr((1, D), F32), b2_o=arr((1, D), F32))
    outs.update(bup_o=arr((1, F), F32), bdn_o=arr((1, D), F32))
    vm = lambda a, t: pltpu.VMEM(a.shape, t)
    scratch = dict(fqkv_v=vm(fqkv, BF), fout_v=vm(fout, BF), fup_v=vm(fup, BF), fdn_v=vm(fdn, BF))
    scratch.update(fqkv_w=vm(fqkv, F32), fout_w=vm(fout, F32), fup_w=vm(fup, F32))
    scratch.update(fdn_w=vm(fdn, F32), out_w=vm(out, F32), gtok_w=vm(gtok, F32))
    scratch.update(sem=pltpu.SemaphoreType.DMA((12,)))
    vmem = pl.BlockSpec(memory_space=pltpu.VMEM)
    hbm = pl.BlockSpec(memory_space=pl.ANY)
    return pl.pallas_call(
        functools.partial(last_kernel, d, (*ins, *outs, *scratch)),
        out_shape=tuple(outs.values()),
        in_specs=[hbm] * 6 + [vmem] * 2,
        out_specs=(hbm,) * 6 + (vmem,) * 8,
        scratch_shapes=list(scratch.values()),
        compiler_params=pltpu.CompilerParams(vmem_limit_bytes=60 * 2**20),
        name="results",
    )(*ins.values())


def call_kernel(d, ins):
    scratch = scratch_of(d)
    I, D, W, F = d.images, d.width, d.local, d.hidden
    vmem = pl.BlockSpec(memory_space=pltpu.VMEM)
    hbm = pl.BlockSpec(memory_space=pl.ANY)
    arr = jax.ShapeDtypeStruct
    outs = dict(
        out_h=arr((I, d.piece, D), F32),
        gtok_h=arr((I, d.piece, D), F32),
        fqkv_h=arr((3, d.part, W), BF),
        fout_h=arr((W, d.part), BF),
        fup_h=arr((d.part, F), BF),
        fdn_h=arr((F, d.part), BF),
        smo=arr((8, D), F32),
        smto=arr((8, D // 4), F32),
    )
    names = (*ins, *outs, *scratch)
    return pl.pallas_call(
        functools.partial(body_kernel, d, names),
        out_shape=tuple(outs.values()),
        in_specs=[hbm] * 15,
        out_specs=(hbm,) * 6 + (vmem,) * 2,
        scratch_shapes=list(scratch.values()),
        compiler_params=pltpu.CompilerParams(
            collective_id=0, has_side_effects=True, vmem_limit_bytes=67043328
        ),
        name="encoder_layer",
    )(*ins.values())


def body(mesh, tokens, pad_mask, ln1_gain, ln1_shift, w_qkv, b_qv, w_out, b_out, ln2_gain, ln2_shift, w_up, b_up, w_down, b_down, cotangent):
    d = dims_of(mesh, tokens.shape, w_out.shape, w_up.shape)
    row = lambda v: v.reshape(1, -1)
    ins = dict(
        tok_h=tokens,
        cot_h=cotangent,
        wqkv_h=w_qkv,
        wout_h=w_out,
        wup_h=w_up,
        wdn_h=w_down,
        mask_h=pad_mask,
        g1_h=row(ln1_gain),
        b1_h=row(ln1_shift),
        bqv_h=b_qv,
        bout_h=row(b_out),
        g2_h=row(ln2_gain),
        b2_h=row(ln2_shift),
        bup_h=row(b_up),
        bdn_h=row(b_down),
    )
    out, gtok, gqkv, gout, gup, gdn, bqv, bout, g1, b1, g2, b2, bup, bdn = call_last(
        d, *call_kernel(d, ins)
    )
    flat = lambda v: v.reshape(-1)
    return (
        out, gtok, gqkv, bqv, gout, flat(bout), flat(g1), flat(b1), flat(g2), flat(b2), gup,
        flat(bup), gdn, flat(bdn),
    )


def solution(mesh):
    return jax.shard_map(
        functools.partial(body, mesh),
        mesh=mesh,
        in_specs=(
            P("shard", "ctx", None),
            P("shard", "ctx"),
            P(),
            P(),
            P(None, "shard", "tp"),
            P(None, "tp"),
            P("tp", "shard"),
            P(),
            P(),
            P(),
            P("shard", "tp"),
            P("tp"),
            P("tp", "shard"),
            P(),
            P("shard", "ctx", None),
        ),
        out_specs=(
            P("shard", "ctx", None),
            P("shard", "ctx", None),
            P(None, "shard", "tp"),
            P(None, "tp"),
            P("tp", "shard"),
            P(),
            P(),
            P(),
            P(),
            P(),
            P("shard", "tp"),
            P("tp"),
            P("tp", "shard"),
            P(),
        ),
        check_vma=False,
    )
```

```python
import functools
import math
import types

import jax
import jax.numpy as jnp
from jax import lax
from jax.experimental import pallas as pl
from jax.experimental.pallas import tpu as pltpu
from jax.sharding import PartitionSpec as P

HD = 64
BIG = 1e30
MESH = pl.DeviceIdType.MESH
BF, F32 = jnp.bfloat16, jnp.float32
RB = 32
TILE = 256


Q, KEY, VAL, OUT, UP, DN = range(6)
Q0, K0, V0, OUT0, UP0, UP1, DN0, DN1 = range(8)
PIECES = (DN0, DN1, UP0, UP1, OUT0, Q0, K0, V0)
(
    LN, FW, KP, QP, KF, AT, P1, SS, SJ, SM, SE, MO, FF, P3, P2, MB, AB, KM, KE, P4, OR, TR,
    GD, GU, GO, GQ, R2, R3, R4, SMA, SMB, FIN,
) = range(32)
CUTS = ((0, 32), (32, 32), (64, 32), (96, 32), (128, 24))
ORDER = (
    (LN, 0), (LN, 2), (FW, KEY), (LN, 1), (KP, 0, 0), (FW, VAL), (KP, 1, 0), (KF, 0, 0), (KP, 0, 2),
    (KP, 0, 1), (FW, Q), (KP, 1, 2), (KP, 1, 1), (KF, 1, 0), (FW, OUT), (QP, 0), (AT, 0), (P1, 0),
    (SS, 1, 0), (QP, 1), (KF, 0, 1), (SM, 1, 0, 0), (SM, 1, 0, 1), (KF, 1, 1), (QP, 2), (KF, 1, 2),
    (SM, 1, 0, 2), (KF, 0, 2), (AT, 1), (SM, 1, 0, 3), (P1, 1), (FW, UP), (SE, 1, 0, 2),
    (SM, 1, 0, 4), (SS, 1, 1), (SE, 1, 0, 1), (SM, 1, 1, 0), (SE, 1, 0, 0), (AT, 2), (SM, 1, 1, 2),
    (SE, 1, 0, 3), (SM, 1, 1, 1), (SM, 1, 1, 3), (P1, 2), (SE, 1, 0, 4), (SE, 1, 1, 2), (SS, 1, 2),
    (SM, 1, 2, 0), (SE, 1, 1, 0), (FW, DN), (MO, 0), (SM, 1, 1, 4), (SM, 1, 2, 1), (SE, 1, 1, 3),
    (SM, 1, 2, 2), (SE, 1, 1, 1), (FF, 0), (SE, 1, 1, 4), (SM, 1, 2, 4), (SE, 1, 2, 0), (P3, 0),
    (SS, 3, 0), (MO, 1), (SM, 1, 2, 3), (FF, 1), (SE, 1, 2, 2), (SE, 1, 2, 1), (SE, 1, 2, 4),
    (P3, 1), (SM, 3, 0, 0), (SE, 1, 2, 3), (SS, 3, 1), (P2, 1), (SM, 3, 0, 1), (P2, 0), (MO, 2),
    (SJ, 2, 0, 2), (FF, 2), (SM, 3, 0, 2), (SM, 3, 0, 3), (P3, 2), (SE, 3, 0, 1), (SM, 3, 0, 4),
    (SS, 3, 2), (GU,), (SJ, 2, 1, 0), (SE, 3, 0, 0), (SM, 3, 1, 1), (SM, 3, 1, 2), (SE, 3, 0, 2),
    (GD,), (SJ, 2, 1, 4), (SM, 3, 1, 0), (R2, UP0), (SJ, 2, 0, 4), (SE, 3, 0, 4), (SJ, 2, 1, 2),
    (SE, 3, 0, 3), (P2, 2), (SM, 2, 0, 2), (SM, 3, 1, 3), (SM, 3, 1, 4), (MB, 0), (R2, UP1),
    (SE, 3, 1, 1), (SM, 3, 2, 0), (SE, 3, 1, 2), (AB, 0), (SE, 3, 1, 0), (R2, DN1), (SJ, 2, 2, 0),
    (SM, 3, 2, 3), (KM, 0), (SE, 3, 1, 3), (SJ, 2, 0, 3), (R3, UP0), (SM, 3, 2, 4), (SE, 3, 1, 4),
    (SM, 3, 2, 1), (SJ, 2, 1, 3), (SJ, 2, 0, 1), (SJ, 2, 2, 2), (MB, 1), (SM, 3, 2, 2),
    (SE, 3, 2, 0), (SE, 3, 2, 3), (SM, 2, 1, 0), (SJ, 2, 2, 3), (SM, 2, 1, 4), (AB, 1),
    (SE, 3, 2, 4), (SM, 2, 0, 4), (KE, 0), (SM, 2, 2, 0), (SE, 3, 2, 1), (R2, DN0), (SE, 3, 2, 2),
    (SM, 2, 0, 3), (P4, 0), (KM, 1), (SS, 4, 0), (SM, 2, 1, 2), (SE, 2, 1, 4), (SE, 2, 1, 0),
    (MB, 2), (SE, 2, 0, 2), (SM, 2, 0, 1), (SJ, 2, 1, 1), (R3, DN1), (SM, 2, 1, 3), (AB, 2),
    (SE, 2, 2, 0), (SM, 2, 2, 2), (SJ, 2, 2, 1), (SE, 2, 0, 3), (KE, 1), (P4, 1), (SE, 2, 0, 4),
    (SE, 2, 0, 1), (SM, 4, 0, 1), (GO,), (GQ, 0), (SJ, 2, 0, 0), (KM, 2), (SE, 2, 1, 2), (R3, DN0),
    (SM, 4, 0, 3), (SM, 4, 0, 4), (SS, 4, 1), (SM, 4, 0, 2), (R2, OUT0), (SE, 4, 0, 1),
    (SM, 2, 1, 1), (SE, 2, 1, 3), (KE, 2), (SE, 2, 2, 2), (SM, 2, 0, 0), (R3, UP1), (SMA,),
    (SM, 4, 0, 0), (SE, 4, 0, 2), (P4, 2), (SM, 2, 2, 1), (SE, 4, 0, 4), (SE, 2, 0, 0), (SS, 4, 2),
    (R2, Q0), (SJ, 2, 2, 4), (SM, 4, 1, 1), (SM, 4, 1, 0), (SE, 2, 1, 1), (SM, 4, 1, 3),
    (SE, 4, 0, 0), (GQ, 1, 2), (SM, 4, 1, 4), (R4, DN1), (R3, OUT0), (SE, 4, 0, 3), (SM, 4, 1, 2),
    (SE, 4, 1, 1), (SM, 4, 2, 1), (R2, V0), (OR, 1), (OR, 0), (R4, DN0), (SE, 4, 1, 0), (R3, Q0),
    (SE, 4, 1, 4), (R4, UP0), (SE, 4, 1, 3), (SM, 4, 2, 2), (TR, 0), (SE, 4, 1, 2), (SM, 4, 2, 4),
    (SM, 4, 2, 0), (SM, 2, 2, 3), (R3, V0), (R2, K0), (SE, 4, 2, 2), (SE, 4, 2, 4), (SM, 4, 2, 3),
    (SE, 4, 2, 0), (SE, 4, 2, 1), (SM, 2, 2, 4), (R3, K0), (R4, UP1), (SE, 4, 2, 3), (SE, 2, 2, 3),
    (R4, OUT0), (TR, 1), (R4, Q0), (TR, 2), (R4, V0), (SE, 2, 2, 4), (SMB,), (SE, 2, 2, 1),
    (R4, K0), (OR, 2), (FIN,),
)


def dot(a, b):
    return lax.dot_general(a, b, (((1,), (0,)), ((), ())), preferred_element_type=F32)


def dot_nt(a, b):
    return lax.dot_general(a, b, (((1,), (1,)), ((), ())), preferred_element_type=F32)


def dot_tn(a, b):
    return lax.dot_general(a, b, (((0,), (0,)), ((), ())), preferred_element_type=F32)


def norm_stats(x):
    centred = x - jnp.mean(x, axis=-1, keepdims=True)
    inv = lax.rsqrt(jnp.mean(centred * centred, axis=-1, keepdims=True) + 1e-06)
    return centred * inv, inv


def norm_back(upstream, unit, inv, gain):
    scaled = upstream * gain
    centre = jnp.mean(scaled, axis=-1, keepdims=True)
    along = jnp.mean(scaled * unit, axis=-1, keepdims=True)
    return inv * (scaled - centre - unit * along)


def fold8(x):
    return jnp.sum(x.reshape(x.shape[0] // 8, 8, x.shape[1]), axis=0)


def aligned(i, m):
    return pl.multiple_of(i, m)


def span(i, n):
    return pl.ds(aligned(i * n, n), n)


class Dims:
    pass


def dims_of(mesh, tokens, w_out, w_up):
    d = Dims()
    d.S, d.C, d.T = (mesh.shape[a] for a in ("shard", "ctx", "tp"))
    assert d.C == 4 and d.T == 4
    d.images, d.piece, d.width = tokens
    d.rows = -(-d.piece // RB) * RB
    d.part = d.width // d.S
    d.local = w_out[0]
    d.hidden = w_up[1]
    d.heads = d.local // HD
    d.keys = d.C * d.rows
    assert d.rows > d.piece
    return d


def scratch_of(d):
    I, R, D, W, F, S, C = d.images, d.rows, d.width, d.local, d.hidden, d.S, d.C
    bf = lambda *shape: pltpu.VMEM(shape, BF)
    f32 = lambda *shape: pltpu.VMEM(shape, F32)
    scratch = dict(
        tok=bf(I, R, D),
        cot=bf(I, R, D),
        maskw=f32(8, TILE),
        first=bf(I, R, D),
        wqkv=bf(3, D, W),
        wout=bf(W, D),
        wup=bf(D, F),
        wdn=bf(F, D),
        q=bf(I, R, W),
        kv=bf(C, I, 2, R, W),
        wts=bf(I, d.heads * R, d.keys),
        att=bf(I, R, W),
        middle=f32(I, R, D),
        second=bf(I, R, D),
        activ=bf(I, R, F),
        actlow=bf(I, R, F),
        mgrad=f32(I, R, D),
        mlow=bf(I, R, D),
        dss=bf(d.heads * R, d.keys),
        qst=bf(d.heads * R, W),
        ost=bf(d.heads * R, W),
        dkv=bf(C, I, 2, R, W),
        rxa=bf(2, I, 2, R, W),
        rxb=bf(I, 2, R, W),
        pg=bf(3, I, R, W),
        acc=f32(8, 8, D),
        sm=f32(8, D),
        smx=f32(S * C, 8, D),
        gqkv=bf(3, D, W),
        gout=bf(W, D),
        gup=bf(D, F),
        gdn=bf(F, D),
        r1q=bf(3, D, W // 2),
        r1o=bf(W // 2, D),
        r1u=bf(2, D, F // 4),
        r1d=bf(2, F // 4, D),
        r2q=bf(3, S, D // S, W // 2),
        r2o=bf(S, W // 2, D // S),
        r2u=bf(2, S, D // S, F // 4),
        r2d=bf(2, S, F // 4, D // S),
        r3q=bf(3, D // S, W // 2),
        r3o=bf(W // 2, D // S),
        r3u=bf(2, D // S, F // 4),
        r3d=bf(2, F // 4, D // S),
        fqkv=bf(3, D // S, W),
        fout=bf(W, D // S),
        fup=bf(D // S, F),
        fdn=bf(F, D // S),
        mask=pltpu.VMEM((I, d.piece), jnp.int32),
        g1=f32(1, D),
        b1=f32(1, D),
        bqv=f32(2, W),
        bout=f32(1, D),
        g2=f32(1, D),
        b2=f32(1, D),
        bup=f32(1, F),
        bdn=f32(1, D),
        smt=f32(8, D // 4),
        smtx=f32(S * C, 8, D // 4),
    )
    full = lambda: bf(I, R, D)
    scratch.update(own1=full(), own2=full(), own3=full(), own4=full())
    scratch.update(tot1=full(), tot2=full(), tot3=full(), tot4=full())
    scratch.update(in01=full(), in02=full(), in03=full())
    scratch.update(in11=full(), in12=full(), in13=full())
    scratch.update(ssem=pltpu.SemaphoreType.DMA((n_sends(d),)))
    scratch.update(rsem=pltpu.SemaphoreType.DMA((n_recvs(d),)))
    scratch.update(lsem=pltpu.SemaphoreType.DMA((7 * I + 13,)))
    return scratch


def n_sends(d):
    return 12 * (d.S - 1) + 8 + 6 + 8 * d.S + 2


def n_recvs(d):
    return 12 * (d.S - 1) + 24 * len(CUTS) + 6 * d.images + 8 * (d.S + 2) + 2


class Net:
    def __init__(self, ssem, rsem, lsem):
        self.ssem, self.rsem, self.lsem = ssem, rsem, lsem
        self.sends, self.recvs, self.locals = {}, {}, 0

    def remote(self, src, dst, device, send, recv):
        return pltpu.make_async_remote_copy(
            src_ref=src,
            dst_ref=dst,
            send_sem=self.ssem.at[self.sends.setdefault(send, len(self.sends))],
            recv_sem=self.rsem.at[self.recvs.setdefault(recv, len(self.recvs))],
            device_id=device,
            device_id_type=MESH,
        )

    def local(self, src, dst):
        n, self.locals = self.locals, self.locals + 1
        return pltpu.make_async_copy(src, dst, self.lsem.at[n])


def body_kernel(d, names, *refs):
    r = types.SimpleNamespace(**dict(zip(names, refs)))
    I, R, D, W, F, S, C = d.images, d.rows, d.width, d.local, d.hidden, d.S, d.C
    piece, part, heads, keys = d.piece, d.part, d.heads, d.keys
    s, c, t = lax.axis_index("shard"), lax.axis_index("ctx"), lax.axis_index("tp")
    core = lax.rem(c, 2)
    mate = c + 1 - 2 * core
    across = lax.rem(c + 2, 4)
    far = lax.rem(mate + 2, 4)
    tmate = t + 1 - 2 * lax.rem(t, 2)
    tpeer = 3 - t
    inner = lax.rem(t + 1, 4) >= 2
    edge = lax.rem(t + 1, 4) < 2
    on_mate, on_across = (s, mate, t), (s, across, t)
    net = Net(r.ssem, r.rsem, r.lsem)
    sent = []

    last = {}

    def go(copy, group=None, whole=None):
        copy.start()
        if group is None:
            sent.append(copy)
        else:
            last[group] = whole

    def drain(key, whole):
        net.remote(whole, whole, on_mate, key, next(iter(net.recvs))).wait_send()

    tail = piece // 16 * 16
    for ref in (r.tot1, r.tot2, r.tot3, r.tot4, r.in01, r.in02, r.in03, r.in11, r.in12, r.in13):
        for i in range(I):
            ref[i, tail:R, :] = jnp.zeros((R - tail, D), BF)
    for i in range(I):
        for n in range(2):
            r.rxb[i, n, tail:R, :] = jnp.zeros((R - tail, W), BF)
            for b in range(2):
                r.rxa[b, i, n, tail:R, :] = jnp.zeros((R - tail, W), BF)

    barrier = pltpu.get_barrier_semaphore()
    pl.semaphore_signal(barrier, inc=1, device_id=(s, c, tmate), device_id_type=MESH)
    for ds in range(S):
        for dc in range(C):
            if ds or dc:
                where = (lax.rem(s + ds, S), lax.rem(c + dc, C), t)
                pl.semaphore_signal(barrier, inc=1, device_id=where, device_id_type=MESH)

    @pl.when(inner)
    def _():
        pl.semaphore_signal(barrier, inc=1, device_id=(s, c, tpeer), device_id_type=MESH)

    loads = {}
    for i in range(I):
        loads[LN, i] = net.local(r.tok_h.at[i], r.tok.at[i, pl.ds(0, piece)])
    vectors = [
        net.local(a, b)
        for a, b in (
            (r.mask_h, r.mask),
            (r.g1_h, r.g1),
            (r.b1_h, r.b1),
            (r.bqv_h, r.bqv),
            (r.bout_h, r.bout),
            (r.g2_h, r.g2),
            (r.b2_h, r.b2),
            (r.bup_h, r.bup),
            (r.bdn_h, r.bdn),
        )
    ]
    rows_s = span(s, part)
    for n in (KEY, VAL, Q):
        loads[n] = net.local(r.wqkv_h.at[n], r.wqkv.at[n, rows_s])
    loads[OUT] = net.local(r.wout_h, r.wout.at[:, rows_s])
    loads[UP] = net.local(r.wup_h, r.wup.at[rows_s])
    loads[DN] = net.local(r.wdn_h, r.wdn.at[:, rows_s])
    for i in range(I):
        loads[FF, i] = net.local(r.cot_h.at[i], r.cot.at[i, pl.ds(0, piece)])
    for copy in (*loads.values(), *vectors):
        copy.start()

    @pl.when(inner)
    def _():
        pl.semaphore_wait(barrier, S * C + 1)

    @pl.when(edge)
    def _():
        pl.semaphore_wait(barrier, S * C)

    def half_of(name, ref, shard, half):
        rows = pl.ds(aligned(shard * part, part), part)
        if name in (Q, KEY, VAL):
            return ref.at[name, rows, span(half, W // 2)]
        if name == OUT:
            return ref.at[pl.ds(aligned(half * (W // 2), W // 2), W // 2), rows]
        if name == UP:
            return ref.at[rows, pl.ds(aligned(half * (F // 2), F // 2), F // 2)]
        return ref.at[pl.ds(aligned(half * (F // 2), F // 2), F // 2), rows]

    def own_half(name, ref, half):
        if name in (Q, KEY, VAL):
            return ref.at[name, :, span(half, W // 2)]
        if name == OUT:
            return ref.at[pl.ds(aligned(half * (W // 2), W // 2), W // 2), :]
        if name == UP:
            return ref.at[:, pl.ds(aligned(half * (F // 2), F // 2), F // 2)]
        return ref.at[pl.ds(aligned(half * (F // 2), F // 2), F // 2), :]

    weights = {
        KEY: (r.wqkv_h, r.wqkv),
        VAL: (r.wqkv_h, r.wqkv),
        Q: (r.wqkv_h, r.wqkv),
        OUT: (r.wout_h, r.wout),
        UP: (r.wup_h, r.wup),
        DN: (r.wdn_h, r.wdn),
    }
    gather, spread = {}, {}
    for name, (source, full) in weights.items():
        for ds in range(1, S):
            to = (lax.rem(s + ds, S), c, t)
            copy = net.remote(
                own_half(name, source, core), half_of(name, full, s, core), to, (FW, name, ds), (FW, name, ds)
            )
            go(copy)
            gather[name, ds] = copy
            owner = lax.rem(s + S - ds, S)
            held = half_of(name, full, owner, core)
            spread[name, ds] = net.remote(held, held, on_mate, (FW, name, -ds), (FW, name, -ds))

    def pass_on(name):
        for ds in range(1, S):
            gather[name, ds].wait_recv()
            go(spread[name, ds])

    arrived = set()

    def weight_ready(name):
        if name in arrived:
            return
        arrived.add(name)
        loads[name].wait()
        for ds in range(1, S):
            spread[name, ds].wait_recv()

    def clear_tail(ref, i):
        if tail < R:
            old = ref[i, pl.ds(tail, R - tail), :].astype(F32)
            row = lax.broadcasted_iota(jnp.int32, old.shape, 0)
            ref[i, pl.ds(tail, R - tail), :] = jnp.where(row < piece - tail, old, 0.0).astype(BF)

    def blocks(fn):
        n = R // 2

        def step(b, _):
            fn(span(b, n))
            return 0

        lax.fori_loop(0, 2, step, 0)

    def tiles(n, fn):
        def step(b, _):
            fn(pl.ds(aligned(b * TILE, TILE), TILE))
            return 0

        lax.fori_loop(0, n // TILE, step, 0)

    r.acc[...] = jnp.zeros_like(r.acc)
    r.sm[...] = jnp.zeros_like(r.sm)
    r.maskw[...] = jnp.zeros_like(r.maskw)
    for copy in vectors:
        copy.wait()
    r.maskw[0:I, 0:piece] = (r.mask[...] > 0).astype(F32)

    def first_norm(i):
        loads[LN, i].wait()
        clear_tail(r.tok, i)

        def rows(w):
            unit, _ = norm_stats(r.tok[i, w, :].astype(F32))
            r.first[i, w, :] = (unit * r.g1[...] + r.b1[...]).astype(BF)

        blocks(rows)

    kv_mate, kv_across, kv_far = {}, {}, {}
    row_w = lax.broadcasted_iota(jnp.int32, (R, W), 0)

    def key_part(n, i):
        weight_ready(KEY + n)
        x = dot(r.first[i], r.wqkv[1 + n])
        if n == 0:
            flags = jnp.broadcast_to(r.maskw[i : i + 1, :], (R, W))
            r.kv[c, i, 0] = jnp.where(row_w == piece, flags, x).astype(BF)
        else:
            r.kv[c, i, 1] = (x + r.bqv[1:2, :]).astype(BF)
        mine = r.kv.at[c, i, n]
        kv_across[n, i] = net.remote(mine, mine, on_across, (KP, 0), (KP, n, i))
        kv_mate[n, i] = net.remote(mine, mine, on_mate, (KP, 1), (KF, i))
        theirs = r.kv.at[across, i, n]
        kv_far[n, i] = net.remote(theirs, theirs, on_mate, (KP, 2), (KF, i))
        go(kv_across[n, i], (KP, 0), r.kv.at[0])
        go(kv_mate[n, i], (KP, 1), r.kv.at[0])

    def queries(i):
        weight_ready(Q)
        r.q[i] = (dot(r.first[i], r.wqkv[0]) + r.bqv[0:1, :]).astype(BF)

    def key_forward(n, i):
        kv_across[n, i].wait_recv()
        go(kv_far[n, i], (KP, 2), r.kv.at[0])

    lane_head = lax.broadcasted_iota(jnp.int32, (R, W), 1) // HD
    scale = 1.0 / math.sqrt(HD)

    def all_keys(i):
        k = jnp.concatenate([r.kv[b, i, 0] for b in range(C)], axis=0)
        v = jnp.concatenate([r.kv[b, i, 1] for b in range(C)], axis=0)
        return k, v

    def key_bias(i):
        row = lax.broadcasted_iota(jnp.int32, (R, W), 0)
        lane = lax.broadcasted_iota(jnp.int32, (R, W), 1)
        lane1 = lax.broadcasted_iota(jnp.int32, (R, 128), 1)
        columns = []
        for b in range(C):
            low = r.kv[b, i, 0, pl.ds(tail, 16), :].astype(F32)
            flags = low[piece - tail : piece - tail + 1, :]
            flag = jnp.sum(jnp.where(row == lane, flags, 0.0), axis=1, keepdims=True)
            columns.append(jnp.where(lane1 == 0, (flag - 1.0) * BIG, 0.0).astype(BF))
        pick = lax.broadcasted_iota(jnp.int32, (16, 128), 1)
        pick = jnp.where(pick == 0, 1.0, 0.0).astype(BF)
        return dot_nt(pick, jnp.concatenate(columns, axis=0))[0:1, :]

    def attention(i):
        pair = r.kv.at[pl.ds(0, 2), i]
        both = net.remote(pair, pair, on_mate, (KP, 1), (KF, i))
        both.wait_recv()
        k, v = all_keys(i)
        bias = key_bias(i)
        q = r.q[i].astype(F32)

        def head(h, total):
            mine = lane_head == h
            qh = jnp.where(mine, q, 0.0).astype(BF)
            scores = dot_nt(qh, k) * scale + bias
            top = jnp.max(scores, axis=-1, keepdims=True)
            e = jnp.exp(scores - top)
            w = (e * (1.0 / jnp.sum(e, axis=-1, keepdims=True))).astype(BF)
            r.wts[i, pl.ds(aligned(h * R, R), R), :] = w
            return jnp.where(mine, dot(w, v), total)

        total = lax.fori_loop(0, heads, head, jnp.zeros((R, W), F32), unroll=True)
        r.att[i] = total.astype(BF)

    hop0, hop1, hop2 = {}, {}, {}

    def sum_plan(k, i):
        own = (r.own1, r.own2, r.own3, r.own4)[k - 1]
        tot = (r.tot1, r.tot2, r.tot3, r.tot4)[k - 1]
        in0 = (r.in01, r.in02, r.in03, r.in01)[k - 1]
        in1 = (r.in11, r.in12, r.in13, r.in11)[k - 1]
        for j, (first, n) in enumerate(CUTS):
            w = pl.ds(first, n)
            a, b = (SM, k, i, j), (SE, k, i, j)
            hop0[k, i, j] = net.remote(own.at[i, w], in0.at[i, w], (s, c, tmate), (SM, k), a)
            hop1[k, i, j] = net.remote(own.at[i, w], in1.at[i, w], (s, c, tpeer), (SM, k), b)
            hop2[k, i, j] = net.remote(tot.at[i, w], tot.at[i, w], (s, c, tmate), (SE, k), a)
        return own, tot, in0, in1

    sums = {(k, i): sum_plan(k, i) for k in range(1, 5) for i in range(I)}

    def add_rows(dst, a, b, i, j):
        first, n = CUTS[j]

        def step(m, _):
            w = pl.ds(aligned(first + m * 16, 16), 16)
            dst[i, w, :] = (a[i, w, :].astype(F32) + b[i, w, :].astype(F32)).astype(BF)
            return 0

        lax.fori_loop(0, -(-n // 16), step, 0)

    def sum_block(k, i, j):
        @pl.when(edge)
        def _():
            hop0[k, i, j].start()

    def sum_start(k, i):
        @pl.when(edge)
        def _():
            for j in range(len(CUTS)):
                hop0[k, i, j].start()

    def sum_mid(k, i, j):
        own, tot, in0, in1 = sums[k, i]

        @pl.when(inner)
        def _():
            hop0[k, i, j].wait_recv()
            add_rows(own, own, in0, i, j)
            hop1[k, i, j].start()

    def sum_end(k, i, j):
        own, tot, in0, in1 = sums[k, i]

        @pl.when(inner)
        def _():
            hop1[k, i, j].wait_recv()
            add_rows(tot, own, in1, i, j)
            hop2[k, i, j].start()

    def sum_got(k, i):
        @pl.when(edge)
        def _():
            for j in range(len(CUTS)):
                hop2[k, i, j].wait_recv()

    def attn_part(i):
        weight_ready(OUT)

        def tile(w):
            r.own1[i, :, w] = dot(r.att[i], r.wout[:, w]).astype(BF)

        tiles(D, tile)

    def middle_of(i):
        sum_got(1, i)

        def rows(w):
            x = r.tok[i, w, :].astype(F32) + r.tot1[i, w, :].astype(F32) + r.bout[...]
            r.middle[i, w, :] = x
            unit, _ = norm_stats(x)
            r.second[i, w, :] = (unit * r.g2[...] + r.b2[...]).astype(BF)

        blocks(rows)

    def feed_forward(i):
        weight_ready(UP)
        weight_ready(DN)
        loads[FF, i].wait()
        clear_tail(r.cot, i)

        def tile(w):
            u = dot(r.second[i], r.wup[:, w]) + r.bup[:, w]
            phi = 0.5 * (1.0 + lax.erf(u * 0.7071067811865476))
            r.activ[i, :, w] = (u * phi).astype(BF)
            slope = phi + u * jnp.exp(-0.5 * u * u) * 0.3989422804014327
            g = dot_nt(r.cot[i], r.wdn[w, :]) * slope
            r.actlow[i, :, w] = g.astype(BF)
            r.acc[6, :, w] += fold8(g)

        tiles(F, tile)

    def norm2_part(i):
        def tile(w):
            r.own3[i, :, w] = dot_nt(r.actlow[i], r.wup[w, :]).astype(BF)

        tiles(D, tile)

    def out_part(i):
        def tile(w):
            r.own2[i, :, w] = dot(r.activ[i], r.wdn[:, w]).astype(BF)

        tiles(D, tile)

    tall = (Q0, K0, V0, UP0, UP1)

    def half_view(piece_id, half, planes, wo, up, dn):
        if piece_id in (Q0, K0, V0):
            return planes.at[piece_id, :, span(half, W // 2)]
        if piece_id == OUT0:
            return wo.at[span(half, W // 2), :]
        n = F // 4
        if piece_id in (UP0, UP1):
            return up.at[:, pl.ds(aligned(half * 2 * n + (piece_id - UP0) * n, n), n)]
        return dn.at[pl.ds(aligned(half * 2 * n + (piece_id - DN0) * n, n), n), :]

    def grad_half(p, half):
        return half_view(p, half, r.gqkv, r.gout, r.gup, r.gdn)

    def final_half(p, half):
        return half_view(p, half, r.fqkv, r.fout, r.fup, r.fdn)

    def slot_of(p, q, o, u, d_):
        if p in (Q0, K0, V0):
            return q.at[p]
        if p == OUT0:
            return o
        return u.at[p - UP0] if p in (UP0, UP1) else d_.at[p - DN0]

    def shard_part(p, ref, shard):
        w = span(shard, part)
        return ref.at[w, :] if p in tall else ref.at[:, w]

    def add_into(dst, a, b):
        def step(k, _):
            w = span(k, RB)
            dst[w, :] = (a[w, :].astype(F32) + b[w, :].astype(F32)).astype(BF)
            return 0

        lax.fori_loop(0, dst.shape[0] // RB, step, 0)

    red = {}

    def reduce1(p):
        red[p, 1] = net.remote(
            grad_half(p, 1 - core), slot_of(p, r.r1q, r.r1o, r.r1u, r.r1d), on_mate, (R3, p), (R2, p)
        )
        red[p, 1].start()

    def reduce2(p):
        r1, r2 = slot_of(p, r.r1q, r.r1o, r.r1u, r.r1d), slot_of(p, r.r2q, r.r2o, r.r2u, r.r2d)
        red[p, 1].wait_recv()
        add_into(r1, grad_half(p, core), r1)
        for ds in range(1, S):
            to = lax.rem(s + ds, S)
            red[p, 2, ds] = net.remote(
                shard_part(p, r1, to), r2.at[ds], (to, c, t), (R2, p, ds), (R3, p, ds)
            )
            red[p, 2, ds].start()

    def reduce3(p):
        r1, r2 = slot_of(p, r.r1q, r.r1o, r.r1u, r.r1d), slot_of(p, r.r2q, r.r2o, r.r2u, r.r2d)
        for ds in range(1, S):
            red[p, 2, ds].wait_recv()
            mine = shard_part(p, r1, s) if ds == 1 else r2.at[0]
            add_into(r2.at[0], mine, r2.at[ds])
        red[p, 1].wait_send()
        red[p, 3] = net.remote(
            r2.at[0], slot_of(p, r.r3q, r.r3o, r.r3u, r.r3d), on_across, (R3, p), (R4, p)
        )
        go(red[p, 3])

    def reduce4(p):
        r2 = slot_of(p, r.r2q, r.r2o, r.r2u, r.r2d)
        red[p, 3].wait_recv()
        mine = final_half(p, core)
        add_into(mine, r2.at[0], slot_of(p, r.r3q, r.r3o, r.r3u, r.r3d))
        for ds in range(1, S):
            red[p, 2, ds].wait_send()
        red[p, 4] = net.remote(mine, mine, on_mate, (R2, p, 1), (FIN, p))
        go(red[p, 4])

    def flat(ref, w=None):
        v = ref[...] if w is None else ref[:, :, w]
        return v.reshape(I * R, v.shape[-1])

    def grad_down():
        def tile(w):
            r.gdn[w, :] = dot_tn(flat(r.activ, w), flat(r.cot)).astype(BF)

        tiles(F, tile)
        reduce1(DN0)
        reduce1(DN1)

    def grad_up():
        def tile(w):
            r.gup[w, :] = dot_tn(flat(r.second, w), flat(r.actlow)).astype(BF)

        tiles(D, tile)
        reduce1(UP0)
        reduce1(UP1)

    def grad_out():
        r.gout[...] = dot_tn(flat(r.att), flat(r.mlow)).astype(BF)
        reduce1(OUT0)

    def grad_proj(*planes):
        def tile(w):
            x = flat(r.first, w)
            for n in planes:
                r.gqkv[n, w, :] = dot_tn(x, flat(r.pg.at[n])).astype(BF)

        tiles(D, tile)
        for n in planes:
            reduce1(Q0 + n)

    def middle_back(i):
        sum_got(3, i)

        def rows(w):
            unit, inv = norm_stats(r.middle[i, w, :])
            n2 = r.tot3[i, w, :].astype(F32)
            up = r.cot[i, w, :].astype(F32)
            g = up + norm_back(n2, unit, inv, r.g2[...])
            r.mgrad[i, w, :] = g
            r.mlow[i, w, :] = g.astype(BF)
            r.acc[1] += fold8(g)
            r.acc[4] += fold8(n2 * unit)
            r.acc[5] += fold8(n2)
            r.acc[7] += fold8(up)

        blocks(rows)

    def attention_back(i):
        k, v = all_keys(i)
        q = r.q[i].astype(F32)
        grad = dot_nt(r.mlow[i], r.wout[...])
        grad = grad.astype(BF).astype(F32)

        def head(h, total):
            mine = lane_head == h
            w = pl.ds(aligned(h * R, R), R)
            gh = jnp.where(mine, grad, 0.0).astype(BF)
            r.ost[w, :] = gh
            r.qst[w, :] = jnp.where(mine, q, 0.0).astype(BF)
            wg = dot_nt(gh, v)
            p = r.wts[i, w, :].astype(F32)
            pw = p * wg
            row_dot = jnp.sum(pw, axis=-1, keepdims=True)
            ds = ((pw - p * row_dot) * scale).astype(BF)
            r.dss[w, :] = ds
            return jnp.where(mine, dot(ds, k), total)

        dq = lax.fori_loop(0, heads, head, jnp.zeros((R, W), F32), unroll=True)
        r.acc[0, :, 0:W] += fold8(dq)
        r.pg[0, i] = dq.astype(BF)
        dk = dot_tn(r.dss[...], r.qst[...]).astype(BF)
        dv = dot_tn(r.wts[i], r.ost[...]).astype(BF)
        for b in range(C):
            r.dkv[b, i, 0] = dk[b * R : (b + 1) * R, :]
            r.dkv[b, i, 1] = dv[b * R : (b + 1) * R, :]
        key_send(i)

    back_mate, back_far, back_across = {}, {}, {}
    real = pl.ds(0, piece)

    def key_send(i):
        back_far[i] = net.remote(
            r.dkv.at[far, i, :, real], r.rxa.at[1, i, :, real], on_mate, (KM, 0), (KM, 0, i)
        )
        back_mate[i] = net.remote(
            r.dkv.at[mate, i, :, real], r.rxa.at[0, i, :, real], on_mate, (KM, 1), (KM, 1, i)
        )
        go(back_far[i], (KM, 0), r.rxb.at[:, :, real])
        go(back_mate[i], (KM, 1), r.rxb.at[:, :, real])

    def key_mid(i):
        back_far[i].wait_recv()
        for n in range(2):
            both = r.dkv[across, i, n].astype(F32) + r.rxa[1, i, n].astype(F32)
            r.rxa[1, i, n] = both.astype(BF)
        back_across[i] = net.remote(
            r.rxa.at[1, i, :, real], r.rxb.at[i, :, real], on_across, (KM, 2), (KM, 2, i)
        )
        go(back_across[i], (KM, 2), r.rxb.at[:, :, real])

    def key_end(i):
        back_mate[i].wait_recv()
        back_across[i].wait_recv()
        for n in range(2):
            both = r.dkv[c, i, n].astype(F32) + r.rxa[0, i, n].astype(F32)
            both = both + r.rxb[i, n].astype(F32)
            r.pg[1 + n, i] = both.astype(BF)
            if n == 1:
                r.acc[0, :, W : 2 * W] += fold8(both)

    def norm1_part(i):
        def tile(w):
            total = dot_nt(r.pg[0, i], r.wqkv[0, w, :])
            total = total + dot_nt(r.pg[1, i], r.wqkv[1, w, :])
            total = total + dot_nt(r.pg[2, i], r.wqkv[2, w, :])
            r.own4[i, :, w] = total.astype(BF)

        tiles(D, tile)

    puts = []

    def out_rows(i):
        sum_got(2, i)

        def rows(w):
            x = r.middle[i, w, :] + r.tot2[i, w, :].astype(F32) + r.bdn[...]
            r.middle[i, w, :] = x

        blocks(rows)
        put = net.local(r.middle.at[i, pl.ds(0, piece)], r.out_h.at[i])
        put.start()
        puts.append(put)

    def token_rows(i):
        sum_got(4, i)

        def rows(w):
            unit, inv = norm_stats(r.tok[i, w, :].astype(F32))
            n1 = r.tot4[i, w, :].astype(F32)
            g = r.mgrad[i, w, :] + norm_back(n1, unit, inv, r.g1[...])
            r.mgrad[i, w, :] = g
            r.acc[2] += fold8(n1 * unit)
            r.acc[3] += fold8(n1)

        blocks(rows)
        put = net.local(r.mgrad.at[i, pl.ds(0, piece)], r.gtok_h.at[i])
        put.start()
        puts.append(put)

    slot = s * C + c
    small = []

    def spread_small(mine, slots, key):
        slots[slot] = mine[...]
        for ds in range(S):
            for dc in range(C):
                if ds or dc:
                    to = (lax.rem(s + ds, S), lax.rem(c + dc, C), t)
                    copy = net.remote(mine, slots.at[slot], to, key, key)
                    copy.start()
        others = slots.at[pl.ds(0, S * C - 1)]
        small.append(net.remote(others, others, on_mate, key, key))

    def small_early():
        for k in (0, 1, 4, 5, 6, 7):
            r.sm[k : k + 1, :] = jnp.sum(r.acc[k], axis=0, keepdims=True)
        spread_small(r.sm, r.smx, SMA)

    def small_late():
        n = D // 4
        for k in range(2):
            total = jnp.sum(r.acc[2 + k], axis=0, keepdims=True)
            for q in range(4):
                r.smt[4 * k + q : 4 * k + q + 1, :] = total[:, q * n : (q + 1) * n]
        spread_small(r.smt, r.smtx, SMB)

    def finish():
        for full, home, pieces in (
            (r.fdn, r.fdn_h, (DN0, DN1)),
            (r.fup, r.fup_h, (UP0, UP1)),
            (r.fout, r.fout_h, (OUT0,)),
            (r.fqkv, r.fqkv_h, (Q0, K0, V0)),
        ):
            for p in pieces:
                red[p, 4].wait_recv()
            put = net.local(full, home)
            put.start()
            puts.append(put)
        for copy in small:
            copy.wait_recv()
        r.smo[...] = lax.fori_loop(1, S * C, lambda n, x: x + r.smx[n], r.smx[0])
        r.smto[...] = lax.fori_loop(1, S * C, lambda n, x: x + r.smtx[n], r.smtx[0])
        for put in puts:
            put.wait()
        for copy in (*sent, *small):
            copy.wait_send()
        for key, whole in last.items():
            drain(key, whole)
        owns, tots = (r.own1, r.own2, r.own3, r.own4), (r.tot1, r.tot2, r.tot3, r.tot4)

        @pl.when(edge)
        def _():
            for k in range(4):
                drain((SM, k + 1), owns[k].at[:, real])

        @pl.when(inner)
        def _():
            for k in range(4):
                drain((SM, k + 1), owns[k].at[:, real])
                drain((SE, k + 1), tots[k].at[:, real])

        assert len(net.sends) <= n_sends(d) and len(net.recvs) <= n_recvs(d)

    steps = {
        LN: first_norm, FW: pass_on, KP: key_part, QP: queries, KF: key_forward,
        AT: attention, P1: attn_part, SS: sum_start, SJ: sum_block, SM: sum_mid, SE: sum_end,
        MO: middle_of, FF: feed_forward, P3: norm2_part, P2: out_part, MB: middle_back,
        AB: attention_back, KM: key_mid, KE: key_end, P4: norm1_part, OR: out_rows,
        TR: token_rows, GD: grad_down, GU: grad_up, GO: grad_out, GQ: grad_proj, R2: reduce2,
        R3: reduce3, R4: reduce4, SMA: small_early, SMB: small_late, FIN: finish,
    }
    for step in ORDER:
        steps[step[0]](*step[1:])


def last_kernel(d, names, *refs):
    r = types.SimpleNamespace(**dict(zip(names, refs)))
    pairs = (
        (r.fdn_i, r.fdn_v, r.fdn_w, r.fdn_o),
        (r.fup_i, r.fup_v, r.fup_w, r.fup_o),
        (r.fqkv_i, r.fqkv_v, r.fqkv_w, r.fqkv_o),
        (r.fout_i, r.fout_v, r.fout_w, r.fout_o),
        (r.out_i, None, r.out_w, r.out_o),
        (r.gtok_i, None, r.gtok_w, r.gtok_o),
    )
    takes = []
    for n, (src, low, wide, dst) in enumerate(pairs):
        takes.append(pltpu.make_async_copy(src, wide if low is None else low, r.sem.at[2 * n]))
        takes[-1].start()
    W, D, F = d.local, d.width, d.hidden
    r.bqv_o[0:1, :] = r.small[0:1, 0:W]
    r.bqv_o[1:2, :] = r.small[0:1, W : 2 * W]
    r.bout_o[...] = r.small[1:2, :]
    r.g2_o[...] = r.small[4:5, :]
    r.b2_o[...] = r.small[5:6, :]
    r.bup_o[...] = r.small[6:7, 0:F]
    r.bdn_o[...] = r.small[7:8, :]
    n4 = D // 4
    for q in range(4):
        w = pl.ds(q * n4, n4)
        r.g1_o[:, w] = r.late[q : q + 1, :]
        r.b1_o[:, w] = r.late[4 + q : 5 + q, :]
    puts = []
    for n, (src, low, wide, dst) in enumerate(pairs):
        takes[n].wait()
        if low is not None:
            planes = [(low.at[k], wide.at[k]) for k in range(3)] if len(low.shape) == 3 else [(low, wide)]
            for a, b in planes:
                step_rows = 64 if a.shape[0] % 64 == 0 else RB

                def step(k, _, a=a, b=b, m=step_rows):
                    w = span(k, m)
                    b[w, :] = a[w, :].astype(F32)
                    return 0

                lax.fori_loop(0, a.shape[0] // step_rows, step, 0)
        puts.append(pltpu.make_async_copy(wide, dst, r.sem.at[2 * n + 1]))
        puts[-1].start()
    for put in puts:
        put.wait()


def call_last(d, out, gtok, fqkv, fout, fup, fdn, small, late):
    I, D, W, F = d.images, d.width, d.local, d.hidden
    arr = jax.ShapeDtypeStruct
    ins = dict(out_i=out, gtok_i=gtok, fqkv_i=fqkv, fout_i=fout, fup_i=fup, fdn_i=fdn)
    ins.update(small=small, late=late)
    outs = dict(out_o=arr(out.shape, F32), gtok_o=arr(gtok.shape, F32))
    outs.update(fqkv_o=arr(fqkv.shape, F32), fout_o=arr(fout.shape, F32))
    outs.update(fup_o=arr(fup.shape, F32), fdn_o=arr(fdn.shape, F32))
    outs.update(bqv_o=arr((2, W), F32), bout_o=arr((1, D), F32), g1_o=arr((1, D), F32))
    outs.update(b1_o=arr((1, D), F32), g2_o=arr((1, D), F32), b2_o=arr((1, D), F32))
    outs.update(bup_o=arr((1, F), F32), bdn_o=arr((1, D), F32))
    vm = lambda a, t: pltpu.VMEM(a.shape, t)
    scratch = dict(fqkv_v=vm(fqkv, BF), fout_v=vm(fout, BF), fup_v=vm(fup, BF), fdn_v=vm(fdn, BF))
    scratch.update(fqkv_w=vm(fqkv, F32), fout_w=vm(fout, F32), fup_w=vm(fup, F32))
    scratch.update(fdn_w=vm(fdn, F32), out_w=vm(out, F32), gtok_w=vm(gtok, F32))
    scratch.update(sem=pltpu.SemaphoreType.DMA((12,)))
    vmem = pl.BlockSpec(memory_space=pltpu.VMEM)
    hbm = pl.BlockSpec(memory_space=pl.ANY)
    return pl.pallas_call(
        functools.partial(last_kernel, d, (*ins, *outs, *scratch)),
        out_shape=tuple(outs.values()),
        in_specs=[hbm] * 6 + [vmem] * 2,
        out_specs=(hbm,) * 6 + (vmem,) * 8,
        scratch_shapes=list(scratch.values()),
        compiler_params=pltpu.CompilerParams(vmem_limit_bytes=60 * 2**20),
        name="results",
    )(*ins.values())


def call_kernel(d, ins):
    scratch = scratch_of(d)
    I, D, W, F = d.images, d.width, d.local, d.hidden
    vmem = pl.BlockSpec(memory_space=pltpu.VMEM)
    hbm = pl.BlockSpec(memory_space=pl.ANY)
    arr = jax.ShapeDtypeStruct
    outs = dict(
        out_h=arr((I, d.piece, D), F32),
        gtok_h=arr((I, d.piece, D), F32),
        fqkv_h=arr((3, d.part, W), BF),
        fout_h=arr((W, d.part), BF),
        fup_h=arr((d.part, F), BF),
        fdn_h=arr((F, d.part), BF),
        smo=arr((8, D), F32),
        smto=arr((8, D // 4), F32),
    )
    names = (*ins, *outs, *scratch)
    return pl.pallas_call(
        functools.partial(body_kernel, d, names),
        out_shape=tuple(outs.values()),
        in_specs=[hbm] * 15,
        out_specs=(hbm,) * 6 + (vmem,) * 2,
        scratch_shapes=list(scratch.values()),
        compiler_params=pltpu.CompilerParams(
            collective_id=0, has_side_effects=True, vmem_limit_bytes=67043328
        ),
        name="encoder_layer",
    )(*ins.values())


def body(mesh, tokens, pad_mask, ln1_gain, ln1_shift, w_qkv, b_qv, w_out, b_out, ln2_gain, ln2_shift, w_up, b_up, w_down, b_down, cotangent):
    d = dims_of(mesh, tokens.shape, w_out.shape, w_up.shape)
    row = lambda v: v.reshape(1, -1)
    ins = dict(
        tok_h=tokens,
        cot_h=cotangent,
        wqkv_h=w_qkv,
        wout_h=w_out,
        wup_h=w_up,
        wdn_h=w_down,
        mask_h=pad_mask,
        g1_h=row(ln1_gain),
        b1_h=row(ln1_shift),
        bqv_h=b_qv,
        bout_h=row(b_out),
        g2_h=row(ln2_gain),
        b2_h=row(ln2_shift),
        bup_h=row(b_up),
        bdn_h=row(b_down),
    )
    out, gtok, gqkv, gout, gup, gdn, bqv, bout, g1, b1, g2, b2, bup, bdn = call_last(
        d, *call_kernel(d, ins)
    )
    flat = lambda v: v.reshape(-1)
    return (
        out, gtok, gqkv, bqv, gout, flat(bout), flat(g1), flat(b1), flat(g2), flat(b2), gup,
        flat(bup), gdn, flat(bdn),
    )


def solution(mesh):
    return jax.shard_map(
        functools.partial(body, mesh),
        mesh=mesh,
        in_specs=(
            P("shard", "ctx", None),
            P("shard", "ctx"),
            P(),
            P(),
            P(None, "shard", "tp"),
            P(None, "tp"),
            P("tp", "shard"),
            P(),
            P(),
            P(),
            P("shard", "tp"),
            P("tp"),
            P("tp", "shard"),
            P(),
            P("shard", "ctx", None),
        ),
        out_specs=(
            P("shard", "ctx", None),
            P("shard", "ctx", None),
            P(None, "shard", "tp"),
            P(None, "tp"),
            P("tp", "shard"),
            P(),
            P(),
            P(),
            P(),
            P(),
            P("shard", "tp"),
            P("tp"),
            P("tp", "shard"),
            P(),
        ),
        check_vma=False,
    )
```

```python
import functools
import math
import types

import jax
import jax.numpy as jnp
from jax import lax
from jax.experimental import pallas as pl
from jax.experimental.pallas import tpu as pltpu
from jax.sharding import PartitionSpec as P

HD = 64
BIG = 1e30
MESH = pl.DeviceIdType.MESH
BF, F32 = jnp.bfloat16, jnp.float32
RB = 32
TILE = 256


Q, KEY, VAL, OUT, UP, DN = range(6)
Q0, K0, V0, OUT0, UP0, UP1, DN0, DN1 = range(8)
PIECES = (DN0, DN1, UP0, UP1, OUT0, Q0, K0, V0)
(
    LN, FW, KP, QP, KF, AT, P1, SS, SJ, SM, SE, MO, FF, P3, P2, MB, AB, KM, KE, P4, OR, TR,
    GD, GU, GO, GQ, R2, R3, R4, SMA, SMB, FIN, AC,
) = range(33)
CUTS = ((0, 32), (32, 32), (64, 32), (96, 32), (128, 24))
ORDER = (
    (FW, KEY), (LN, 0), (KP, 0, 0), (LN, 2), (FW, VAL), (KP, 1, 0), (FW, Q), (LN, 1), (KF, 0, 0),
    (KF, 1, 0), (KP, 1, 1), (QP, 0), (FW, OUT), (KP, 0, 1), (AT, 0), (P1, 0), (SM, 1, 0, 1),
    (SM, 1, 0, 0), (SS, 1, 0), (KP, 0, 2), (KF, 1, 1), (SM, 1, 0, 2), (KF, 0, 1), (QP, 1),
    (KP, 1, 2), (SM, 1, 0, 3), (AT, 1), (SM, 1, 0, 4), (P1, 1), (SS, 1, 1), (SM, 1, 1, 0),
    (SE, 1, 0, 2), (SE, 1, 0, 1), (SE, 1, 0, 4), (SE, 1, 0, 0), (SM, 1, 1, 2), (KF, 0, 2),
    (SE, 1, 0, 3), (KF, 1, 2), (QP, 2), (SE, 1, 1, 0), (SM, 1, 1, 1), (SM, 1, 1, 3), (AT, 2),
    (P1, 2), (SS, 1, 2), (FW, UP), (SM, 1, 1, 4), (SE, 1, 1, 2), (SM, 1, 2, 0), (FW, DN),
    (SM, 1, 2, 2), (MO, 0), (SE, 1, 1, 3), (SE, 1, 1, 1), (FF, 0, 0), (SE, 1, 1, 4), (SM, 1, 2, 3),
    (FF, 0, 1), (SE, 1, 2, 0), (P3, 0, 0), (P3, 0, 1), (SM, 1, 2, 1), (SS, 3, 0), (P2, 0, 0),
    (SE, 1, 2, 2), (SM, 1, 2, 4), (MO, 1), (FF, 1, 0), (FF, 1, 1), (SE, 1, 2, 3), (P3, 1, 1),
    (P2, 0, 1), (SM, 3, 0, 0), (SE, 1, 2, 4), (SE, 1, 2, 1), (SM, 3, 0, 1), (P3, 1, 0), (SS, 3, 1),
    (P2, 1, 1), (SJ, 2, 0, 3), (MO, 2), (SM, 3, 0, 2), (SM, 3, 0, 3), (SM, 3, 0, 4), (SE, 3, 0, 0),
    (FF, 2, 0), (FF, 2, 1), (SM, 3, 1, 0), (P3, 2, 0), (SE, 3, 0, 2), (P3, 2, 1), (SM, 3, 1, 1),
    (SS, 3, 2), (SE, 3, 0, 1), (GU, 0), (GU, 1), (GD, 1), (SE, 3, 0, 4), (SM, 3, 1, 2), (P2, 1, 0),
    (SE, 3, 0, 3), (SE, 3, 1, 0), (R2, UP0), (SJ, 2, 1, 4), (SM, 3, 1, 3), (SJ, 2, 0, 1), (MB, 0),
    (SM, 3, 1, 4), (SJ, 2, 1, 1), (AB, 0), (SE, 3, 1, 2), (SM, 2, 0, 3), (AC, 0), (SE, 3, 1, 3),
    (SJ, 2, 0, 0), (SM, 3, 2, 0), (P2, 2, 0), (KM, 0), (P2, 2, 1), (SE, 3, 1, 1), (SM, 3, 2, 2),
    (R2, UP1), (SM, 3, 2, 1), (R2, DN1), (SE, 3, 1, 4), (GD, 0), (SJ, 2, 1, 2), (MB, 1),
    (SM, 3, 2, 4), (SE, 3, 2, 0), (SJ, 2, 2, 2), (R3, UP0), (SJ, 2, 1, 0), (SM, 3, 2, 3),
    (SJ, 2, 1, 3), (SE, 3, 2, 2), (AB, 1), (SE, 3, 2, 1), (KE, 0), (SM, 2, 0, 1), (SM, 2, 1, 4),
    (SM, 2, 1, 1), (SE, 3, 2, 4), (AC, 1), (SM, 2, 0, 0), (SE, 3, 2, 3), (SE, 2, 0, 3), (P4, 0, 0),
    (SJ, 2, 0, 4), (R2, DN0), (P4, 0, 1), (SM, 2, 1, 2), (SE, 2, 0, 1), (SS, 4, 0), (KM, 1),
    (MB, 2), (SM, 2, 2, 2), (SE, 2, 1, 4), (AB, 2), (AC, 2), (SM, 2, 1, 0), (SE, 2, 1, 1),
    (SJ, 2, 0, 2), (SM, 2, 1, 3), (GQ, 0), (SE, 2, 1, 2), (KM, 2), (KE, 1), (SM, 4, 0, 0),
    (SE, 2, 0, 0), (P4, 1, 1), (SM, 2, 0, 4), (SE, 2, 1, 0), (P4, 1, 0), (SE, 2, 1, 3), (SS, 4, 1),
    (R3, UP1), (SJ, 2, 2, 4), (GO,), (SM, 4, 0, 1), (SE, 4, 0, 0), (SE, 2, 0, 4), (KE, 2),
    (SM, 4, 0, 4), (SE, 2, 2, 2), (P4, 2, 1), (SM, 2, 0, 2), (SM, 4, 0, 2), (SM, 4, 0, 3), (OR, 1),
    (R3, DN0), (R4, UP0), (SE, 4, 0, 1), (GQ, 1, 2), (R3, DN1), (R2, Q0), (SE, 4, 0, 4),
    (SM, 4, 1, 2), (SM, 4, 1, 1), (SE, 2, 0, 2), (P4, 2, 0), (SM, 4, 1, 0), (R2, V0), (SE, 4, 0, 2),
    (SM, 4, 1, 3), (SE, 4, 0, 3), (SS, 4, 2), (SM, 2, 2, 4), (SM, 4, 1, 4), (SE, 4, 1, 2),
    (SE, 4, 1, 1), (SJ, 2, 2, 1), (OR, 0), (SE, 4, 1, 0), (SE, 4, 1, 3), (R2, OUT0), (SM, 4, 2, 2),
    (R4, UP1), (SM, 4, 2, 1), (R2, K0), (SM, 4, 2, 0), (SJ, 2, 2, 3), (R3, V0), (SE, 2, 2, 4),
    (SJ, 2, 2, 0), (TR, 0), (R3, Q0), (SE, 4, 1, 4), (SM, 4, 2, 3), (SM, 4, 2, 4), (SE, 4, 2, 2),
    (SM, 2, 2, 3), (SE, 4, 2, 1), (R4, DN0), (SM, 2, 2, 0), (R3, OUT0), (SE, 4, 2, 0), (R4, V0),
    (SM, 2, 2, 1), (SE, 4, 2, 3), (R4, DN1), (R3, K0), (TR, 1), (SE, 4, 2, 4), (SE, 2, 2, 3),
    (SMA,), (R4, Q0), (TR, 2), (SMB,), (R4, OUT0), (SE, 2, 2, 0), (SE, 2, 2, 1), (R4, K0), (OR, 2),
    (FIN,),
)


def dot(a, b):
    return lax.dot_general(a, b, (((1,), (0,)), ((), ())), preferred_element_type=F32)


def dot_nt(a, b):
    return lax.dot_general(a, b, (((1,), (1,)), ((), ())), preferred_element_type=F32)


def dot_tn(a, b):
    return lax.dot_general(a, b, (((0,), (0,)), ((), ())), preferred_element_type=F32)


def norm_stats(x):
    centred = x - jnp.mean(x, axis=-1, keepdims=True)
    inv = lax.rsqrt(jnp.mean(centred * centred, axis=-1, keepdims=True) + 1e-06)
    return centred * inv, inv


def norm_back(upstream, unit, inv, gain):
    scaled = upstream * gain
    centre = jnp.mean(scaled, axis=-1, keepdims=True)
    along = jnp.mean(scaled * unit, axis=-1, keepdims=True)
    return inv * (scaled - centre - unit * along)


def fold8(x):
    return jnp.sum(x.reshape(x.shape[0] // 8, 8, x.shape[1]), axis=0)


def aligned(i, m):
    return pl.multiple_of(i, m)


def span(i, n):
    return pl.ds(aligned(i * n, n), n)


class Dims:
    pass


def dims_of(mesh, tokens, w_out, w_up):
    d = Dims()
    d.S, d.C, d.T = (mesh.shape[a] for a in ("shard", "ctx", "tp"))
    assert d.C == 4 and d.T == 4
    d.images, d.piece, d.width = tokens
    d.rows = -(-d.piece // RB) * RB
    d.part = d.width // d.S
    d.local = w_out[0]
    d.hidden = w_up[1]
    d.heads = d.local // HD
    d.keys = d.C * d.rows
    assert d.rows > d.piece
    return d


def scratch_of(d):
    I, R, D, W, F, S, C = d.images, d.rows, d.width, d.local, d.hidden, d.S, d.C
    bf = lambda *shape: pltpu.VMEM(shape, BF)
    f32 = lambda *shape: pltpu.VMEM(shape, F32)
    scratch = dict(
        tok=bf(I, R, D),
        cot=bf(I, R, D),
        maskw=f32(8, TILE),
        first=bf(I, R, D),
        wqkv=bf(3, D, W),
        wout=bf(W, D),
        wup=bf(D, F),
        wdn=bf(F, D),
        q=bf(I, R, W),
        kv=bf(C, I, 2, R, W),
        wts=bf(I, d.heads * R, d.keys),
        att=bf(I, R, W),
        middle=f32(I, R, D),
        second=bf(I, R, D),
        activ=bf(I, R, F),
        actlow=bf(I, R, F),
        mgrad=f32(I, R, D),
        mlow=bf(I, R, D),
        dss=bf(d.heads * R, d.keys),
        qst=bf(d.heads * R, W),
        ost=bf(d.heads * R, W),
        dkv=bf(C, I, 2, R, W),
        rxa=bf(2, I, 2, R, W),
        rxb=bf(I, 2, R, W),
        pg=bf(3, I, R, W),
        acc=f32(8, 8, D),
        sm=f32(8, D),
        smx=f32(S * C, 8, D),
        gqkv=bf(3, D, W),
        gout=bf(W, D),
        gup=bf(D, F),
        gdn=bf(F, D),
        r1q=bf(3, D, W // 2),
        r1o=bf(W // 2, D),
        r1u=bf(2, D, F // 4),
        r1d=bf(2, F // 4, D),
        r2q=bf(3, S, D // S, W // 2),
        r2o=bf(S, W // 2, D // S),
        r2u=bf(2, S, D // S, F // 4),
        r2d=bf(2, S, F // 4, D // S),
        r3q=bf(3, D // S, W // 2),
        r3o=bf(W // 2, D // S),
        r3u=bf(2, D // S, F // 4),
        r3d=bf(2, F // 4, D // S),
        fqkv=bf(3, D // S, W),
        fout=bf(W, D // S),
        fup=bf(D // S, F),
        fdn=bf(F, D // S),
        mask=pltpu.VMEM((I, d.piece), jnp.int32),
        g1=f32(1, D),
        b1=f32(1, D),
        bqv=f32(2, W),
        bout=f32(1, D),
        g2=f32(1, D),
        b2=f32(1, D),
        bup=f32(1, F),
        bdn=f32(1, D),
        smt=f32(8, D // 4),
        smtx=f32(S * C, 8, D // 4),
    )
    full = lambda: bf(I, R, D)
    scratch.update(own1=full(), own2=full(), own3=full(), own4=full())
    scratch.update(tot1=full(), tot2=full(), tot3=full(), tot4=full())
    scratch.update(in01=full(), in02=full(), in03=full())
    scratch.update(in11=full(), in12=full(), in13=full())
    scratch.update(ssem=pltpu.SemaphoreType.DMA((n_sends(d),)))
    scratch.update(rsem=pltpu.SemaphoreType.DMA((n_recvs(d),)))
    scratch.update(lsem=pltpu.SemaphoreType.DMA((7 * I + 13,)))
    return scratch


def n_sends(d):
    return 12 * (d.S - 1) + 8 + 6 + 8 * d.S + 2


def n_recvs(d):
    return 12 * (d.S - 1) + 18 * len(CUTS) + 6 * d.images + 8 * (d.S + 2) + 2


class Net:
    def __init__(self, ssem, rsem, lsem):
        self.ssem, self.rsem, self.lsem = ssem, rsem, lsem
        self.sends, self.recvs, self.locals = {}, {}, 0

    def remote(self, src, dst, device, send, recv):
        return pltpu.make_async_remote_copy(
            src_ref=src,
            dst_ref=dst,
            send_sem=self.ssem.at[self.sends.setdefault(send, len(self.sends))],
            recv_sem=self.rsem.at[self.recvs.setdefault(recv, len(self.recvs))],
            device_id=device,
            device_id_type=MESH,
        )

    def local(self, src, dst):
        n, self.locals = self.locals, self.locals + 1
        return pltpu.make_async_copy(src, dst, self.lsem.at[n])


def body_kernel(d, names, *refs):
    r = types.SimpleNamespace(**dict(zip(names, refs)))
    I, R, D, W, F, S, C = d.images, d.rows, d.width, d.local, d.hidden, d.S, d.C
    piece, part, heads, keys = d.piece, d.part, d.heads, d.keys
    s, c, t = lax.axis_index("shard"), lax.axis_index("ctx"), lax.axis_index("tp")
    core = lax.rem(c, 2)
    mate = c + 1 - 2 * core
    across = lax.rem(c + 2, 4)
    far = lax.rem(mate + 2, 4)
    tmate = t + 1 - 2 * lax.rem(t, 2)
    tpeer = 3 - t
    inner = lax.rem(t + 1, 4) >= 2
    edge = lax.rem(t + 1, 4) < 2
    on_mate, on_across = (s, mate, t), (s, across, t)
    net = Net(r.ssem, r.rsem, r.lsem)
    sent = []

    last = {}

    def go(copy, group=None, whole=None):
        copy.start()
        if group is None:
            sent.append(copy)
        else:
            last[group] = whole

    def drain(key, whole):
        net.remote(whole, whole, on_mate, key, next(iter(net.recvs))).wait_send()

    tail = piece // 16 * 16
    for ref in (r.tot1, r.tot2, r.tot3, r.tot4, r.in01, r.in02, r.in03, r.in11, r.in12, r.in13):
        for i in range(I):
            ref[i, tail:R, :] = jnp.zeros((R - tail, D), BF)
    for i in range(I):
        for n in range(2):
            r.rxb[i, n, tail:R, :] = jnp.zeros((R - tail, W), BF)
            for b in range(2):
                r.rxa[b, i, n, tail:R, :] = jnp.zeros((R - tail, W), BF)

    barrier = pltpu.get_barrier_semaphore()
    pl.semaphore_signal(barrier, inc=1, device_id=(s, c, tmate), device_id_type=MESH)
    for ds in range(S):
        for dc in range(C):
            if ds or dc:
                where = (lax.rem(s + ds, S), lax.rem(c + dc, C), t)
                pl.semaphore_signal(barrier, inc=1, device_id=where, device_id_type=MESH)

    @pl.when(inner)
    def _():
        pl.semaphore_signal(barrier, inc=1, device_id=(s, c, tpeer), device_id_type=MESH)

    loads = {}
    for i in range(I):
        loads[LN, i] = net.local(r.tok_h.at[i], r.tok.at[i, pl.ds(0, piece)])
    vectors = [
        net.local(a, b)
        for a, b in (
            (r.mask_h, r.mask),
            (r.g1_h, r.g1),
            (r.b1_h, r.b1),
            (r.bqv_h, r.bqv),
            (r.bout_h, r.bout),
            (r.g2_h, r.g2),
            (r.b2_h, r.b2),
            (r.bup_h, r.bup),
            (r.bdn_h, r.bdn),
        )
    ]
    rows_s = span(s, part)
    for n in (KEY, VAL, Q):
        loads[n] = net.local(r.wqkv_h.at[n], r.wqkv.at[n, rows_s])
    loads[OUT] = net.local(r.wout_h, r.wout.at[:, rows_s])
    loads[UP] = net.local(r.wup_h, r.wup.at[rows_s])
    loads[DN] = net.local(r.wdn_h, r.wdn.at[:, rows_s])
    for i in range(I):
        loads[FF, i] = net.local(r.cot_h.at[i], r.cot.at[i, pl.ds(0, piece)])
    for copy in (*loads.values(), *vectors):
        copy.start()

    @pl.when(inner)
    def _():
        pl.semaphore_wait(barrier, S * C + 1)

    @pl.when(edge)
    def _():
        pl.semaphore_wait(barrier, S * C)

    def half_of(name, ref, shard, half):
        rows = pl.ds(aligned(shard * part, part), part)
        if name in (Q, KEY, VAL):
            return ref.at[name, rows, span(half, W // 2)]
        if name == OUT:
            return ref.at[pl.ds(aligned(half * (W // 2), W // 2), W // 2), rows]
        if name == UP:
            return ref.at[rows, pl.ds(aligned(half * (F // 2), F // 2), F // 2)]
        return ref.at[pl.ds(aligned(half * (F // 2), F // 2), F // 2), rows]

    def own_half(name, ref, half):
        if name in (Q, KEY, VAL):
            return ref.at[name, :, span(half, W // 2)]
        if name == OUT:
            return ref.at[pl.ds(aligned(half * (W // 2), W // 2), W // 2), :]
        if name == UP:
            return ref.at[:, pl.ds(aligned(half * (F // 2), F // 2), F // 2)]
        return ref.at[pl.ds(aligned(half * (F // 2), F // 2), F // 2), :]

    weights = {
        KEY: (r.wqkv_h, r.wqkv),
        VAL: (r.wqkv_h, r.wqkv),
        Q: (r.wqkv_h, r.wqkv),
        OUT: (r.wout_h, r.wout),
        UP: (r.wup_h, r.wup),
        DN: (r.wdn_h, r.wdn),
    }
    gather, spread = {}, {}
    for name, (source, full) in weights.items():
        for ds in range(1, S):
            to = (lax.rem(s + ds, S), c, t)
            copy = net.remote(
                own_half(name, source, core), half_of(name, full, s, core), to, (FW, name, ds), (FW, name, ds)
            )
            go(copy)
            gather[name, ds] = copy
            owner = lax.rem(s + S - ds, S)
            held = half_of(name, full, owner, core)
            spread[name, ds] = net.remote(held, held, on_mate, (FW, name, -ds), (FW, name, -ds))

    def pass_on(name):
        for ds in range(1, S):
            gather[name, ds].wait_recv()
            go(spread[name, ds])

    arrived = set()

    def weight_ready(name):
        if name in arrived:
            return
        arrived.add(name)
        loads[name].wait()
        for ds in range(1, S):
            spread[name, ds].wait_recv()

    def clear_tail(ref, i):
        if tail < R:
            old = ref[i, pl.ds(tail, R - tail), :].astype(F32)
            row = lax.broadcasted_iota(jnp.int32, old.shape, 0)
            ref[i, pl.ds(tail, R - tail), :] = jnp.where(row < piece - tail, old, 0.0).astype(BF)

    def blocks(fn):
        n = R // 2

        def step(b, _):
            fn(span(b, n))
            return 0

        lax.fori_loop(0, 2, step, 0)

    def tiles(n, fn, h=None, stride=1):
        count = n // TILE
        first = 0 if h is None else h * (count // 2 if stride == 1 else 1)

        def step(b, _):
            fn(span(first + b * stride, TILE))
            return 0

        lax.fori_loop(0, count if h is None else count // 2, step, 0)

    r.acc[...] = jnp.zeros_like(r.acc)
    r.sm[...] = jnp.zeros_like(r.sm)
    r.maskw[...] = jnp.zeros_like(r.maskw)
    for copy in vectors:
        copy.wait()
    r.maskw[0:I, 0:piece] = (r.mask[...] > 0).astype(F32)

    def first_norm(i):
        loads[LN, i].wait()
        clear_tail(r.tok, i)

        def rows(w):
            unit, _ = norm_stats(r.tok[i, w, :].astype(F32))
            r.first[i, w, :] = (unit * r.g1[...] + r.b1[...]).astype(BF)

        blocks(rows)

    kv_mate, kv_across, kv_far = {}, {}, {}
    row_w = lax.broadcasted_iota(jnp.int32, (R, W), 0)

    def key_part(n, i):
        weight_ready(KEY + n)
        x = dot(r.first[i], r.wqkv[1 + n])
        if n == 0:
            flags = jnp.broadcast_to(r.maskw[i : i + 1, :], (R, W))
            r.kv[c, i, 0] = jnp.where(row_w == piece, flags, x).astype(BF)
        else:
            r.kv[c, i, 1] = (x + r.bqv[1:2, :]).astype(BF)
        mine = r.kv.at[c, i, n]
        kv_across[n, i] = net.remote(mine, mine, on_across, (KP, 0), (KP, n, i))
        kv_mate[n, i] = net.remote(mine, mine, on_mate, (KP, 1), (KF, i))
        theirs = r.kv.at[across, i, n]
        kv_far[n, i] = net.remote(theirs, theirs, on_mate, (KP, 2), (KF, i))
        go(kv_across[n, i], (KP, 0), r.kv.at[0])
        go(kv_mate[n, i], (KP, 1), r.kv.at[0])

    def queries(i):
        weight_ready(Q)
        r.q[i] = (dot(r.first[i], r.wqkv[0]) + r.bqv[0:1, :]).astype(BF)

    def key_forward(n, i):
        kv_across[n, i].wait_recv()
        go(kv_far[n, i], (KP, 2), r.kv.at[0])

    lane_head = lax.broadcasted_iota(jnp.int32, (R, W), 1) // HD
    scale = 1.0 / math.sqrt(HD)

    def all_keys(i):
        k = jnp.concatenate([r.kv[b, i, 0] for b in range(C)], axis=0)
        v = jnp.concatenate([r.kv[b, i, 1] for b in range(C)], axis=0)
        return k, v

    def key_bias(i):
        row = lax.broadcasted_iota(jnp.int32, (R, W), 0)
        lane = lax.broadcasted_iota(jnp.int32, (R, W), 1)
        lane1 = lax.broadcasted_iota(jnp.int32, (R, 128), 1)
        columns = []
        for b in range(C):
            low = r.kv[b, i, 0, pl.ds(tail, 16), :].astype(F32)
            flags = low[piece - tail : piece - tail + 1, :]
            flag = jnp.sum(jnp.where(row == lane, flags, 0.0), axis=1, keepdims=True)
            columns.append(jnp.where(lane1 == 0, (flag - 1.0) * BIG, 0.0).astype(BF))
        pick = lax.broadcasted_iota(jnp.int32, (16, 128), 1)
        pick = jnp.where(pick == 0, 1.0, 0.0).astype(BF)
        return dot_nt(pick, jnp.concatenate(columns, axis=0))[0:1, :]

    def attention(i):
        pair = r.kv.at[pl.ds(0, 2), i]
        both = net.remote(pair, pair, on_mate, (KP, 1), (KF, i))
        both.wait_recv()
        k, v = all_keys(i)
        bias = key_bias(i)
        q = r.q[i].astype(F32)

        def head(h, total):
            mine = lane_head == h
            qh = jnp.where(mine, q, 0.0).astype(BF)
            scores = dot_nt(qh, k) * scale + bias
            top = jnp.max(scores, axis=-1, keepdims=True)
            e = jnp.exp(scores - top)
            w = (e * (1.0 / jnp.sum(e, axis=-1, keepdims=True))).astype(BF)
            r.wts[i, pl.ds(aligned(h * R, R), R), :] = w
            return jnp.where(mine, dot(w, v), total)

        total = lax.fori_loop(0, heads, head, jnp.zeros((R, W), F32), unroll=True)
        r.att[i] = total.astype(BF)

    hop0, hop1, hop2 = {}, {}, {}

    def lanes_of(k):
        return 1 if k == 4 else k

    def sum_plan(k, i):
        own = (r.own1, r.own2, r.own3, r.own4)[k - 1]
        tot = (r.tot1, r.tot2, r.tot3, r.tot4)[k - 1]
        in0 = (r.in01, r.in02, r.in03, r.in01)[k - 1]
        in1 = (r.in11, r.in12, r.in13, r.in11)[k - 1]
        for j, (first, n) in enumerate(CUTS):
            w = pl.ds(first, n)
            a, b = (SM, lanes_of(k), i, j), (SE, lanes_of(k), i, j)
            hop0[k, i, j] = net.remote(own.at[i, w], in0.at[i, w], (s, c, tmate), (SM, k), a)
            hop1[k, i, j] = net.remote(own.at[i, w], in1.at[i, w], (s, c, tpeer), (SM, k), b)
            hop2[k, i, j] = net.remote(tot.at[i, w], tot.at[i, w], (s, c, tmate), (SE, k), a)
        return own, tot, in0, in1

    sums = {(k, i): sum_plan(k, i) for k in range(1, 5) for i in range(I)}

    def add_rows(dst, a, b, i, j):
        first, n = CUTS[j]

        def step(m, _):
            w = pl.ds(aligned(first + m * 16, 16), 16)
            dst[i, w, :] = (a[i, w, :].astype(F32) + b[i, w, :].astype(F32)).astype(BF)
            return 0

        lax.fori_loop(0, -(-n // 16), step, 0)

    def sum_block(k, i, j):
        @pl.when(edge)
        def _():
            hop0[k, i, j].start()

    def sum_start(k, i):
        @pl.when(edge)
        def _():
            for j in range(len(CUTS)):
                hop0[k, i, j].start()

    def sum_mid(k, i, j):
        own, tot, in0, in1 = sums[k, i]

        @pl.when(inner)
        def _():
            hop0[k, i, j].wait_recv()
            add_rows(own, own, in0, i, j)
            hop1[k, i, j].start()

    def sum_end(k, i, j):
        own, tot, in0, in1 = sums[k, i]

        @pl.when(inner)
        def _():
            hop1[k, i, j].wait_recv()
            add_rows(tot, own, in1, i, j)
            hop2[k, i, j].start()

    def sum_got(k, i):
        @pl.when(edge)
        def _():
            for j in range(len(CUTS)):
                hop2[k, i, j].wait_recv()

    def attn_part(i):
        weight_ready(OUT)

        def tile(w):
            r.own1[i, :, w] = dot(r.att[i], r.wout[:, w]).astype(BF)

        tiles(D, tile)

    def middle_of(i):
        sum_got(1, i)

        def rows(w):
            x = r.tok[i, w, :].astype(F32) + r.tot1[i, w, :].astype(F32) + r.bout[...]
            r.middle[i, w, :] = x
            unit, _ = norm_stats(x)
            r.second[i, w, :] = (unit * r.g2[...] + r.b2[...]).astype(BF)

        blocks(rows)

    def feed_forward(i, h):
        weight_ready(UP)
        weight_ready(DN)
        if h == 0:
            loads[FF, i].wait()
            clear_tail(r.cot, i)

        def tile(w):
            u = dot(r.second[i], r.wup[:, w]) + r.bup[:, w]
            phi = 0.5 * (1.0 + lax.erf(u * 0.7071067811865476))
            r.activ[i, :, w] = (u * phi).astype(BF)
            slope = phi + u * jnp.exp(-0.5 * u * u) * 0.3989422804014327
            g = dot_nt(r.cot[i], r.wdn[w, :]) * slope
            r.actlow[i, :, w] = g.astype(BF)
            r.acc[6, :, w] += fold8(g)

        tiles(F, tile, h)

    def norm2_part(i, h):
        def tile(w):
            r.own3[i, :, w] = dot_nt(r.actlow[i], r.wup[w, :]).astype(BF)

        tiles(D, tile, h)

    def out_part(i, h):
        def tile(w):
            r.own2[i, :, w] = dot(r.activ[i], r.wdn[:, w]).astype(BF)

        tiles(D, tile, h)

    tall = (Q0, K0, V0, UP0, UP1)

    def half_view(piece_id, half, planes, wo, up, dn):
        if piece_id in (Q0, K0, V0):
            return planes.at[piece_id, :, span(half, W // 2)]
        if piece_id == OUT0:
            return wo.at[span(half, W // 2), :]
        n = F // 4
        if piece_id in (UP0, UP1):
            return up.at[:, pl.ds(aligned(half * 2 * n + (piece_id - UP0) * n, n), n)]
        return dn.at[pl.ds(aligned(half * 2 * n + (piece_id - DN0) * n, n), n), :]

    def grad_half(p, half):
        return half_view(p, half, r.gqkv, r.gout, r.gup, r.gdn)

    def final_half(p, half):
        return half_view(p, half, r.fqkv, r.fout, r.fup, r.fdn)

    def slot_of(p, q, o, u, d_):
        if p in (Q0, K0, V0):
            return q.at[p]
        if p == OUT0:
            return o
        return u.at[p - UP0] if p in (UP0, UP1) else d_.at[p - DN0]

    def shard_part(p, ref, shard):
        w = span(shard, part)
        return ref.at[w, :] if p in tall else ref.at[:, w]

    def add_into(dst, a, b):
        def step(k, _):
            w = span(k, RB)
            dst[w, :] = (a[w, :].astype(F32) + b[w, :].astype(F32)).astype(BF)
            return 0

        lax.fori_loop(0, dst.shape[0] // RB, step, 0)

    red = {}

    def reduce1(p):
        red[p, 1] = net.remote(
            grad_half(p, 1 - core), slot_of(p, r.r1q, r.r1o, r.r1u, r.r1d), on_mate, (R3, p), (R2, p)
        )
        red[p, 1].start()

    def reduce2(p):
        r1, r2 = slot_of(p, r.r1q, r.r1o, r.r1u, r.r1d), slot_of(p, r.r2q, r.r2o, r.r2u, r.r2d)
        red[p, 1].wait_recv()
        add_into(r1, grad_half(p, core), r1)
        for ds in range(1, S):
            to = lax.rem(s + ds, S)
            red[p, 2, ds] = net.remote(
                shard_part(p, r1, to), r2.at[ds], (to, c, t), (R2, p, ds), (R3, p, ds)
            )
            red[p, 2, ds].start()

    def reduce3(p):
        r1, r2 = slot_of(p, r.r1q, r.r1o, r.r1u, r.r1d), slot_of(p, r.r2q, r.r2o, r.r2u, r.r2d)
        for ds in range(1, S):
            red[p, 2, ds].wait_recv()
            mine = shard_part(p, r1, s) if ds == 1 else r2.at[0]
            add_into(r2.at[0], mine, r2.at[ds])
        red[p, 1].wait_send()
        red[p, 3] = net.remote(
            r2.at[0], slot_of(p, r.r3q, r.r3o, r.r3u, r.r3d), on_across, (R3, p), (R4, p)
        )
        go(red[p, 3])

    def reduce4(p):
        r2 = slot_of(p, r.r2q, r.r2o, r.r2u, r.r2d)
        red[p, 3].wait_recv()
        mine = final_half(p, core)
        add_into(mine, r2.at[0], slot_of(p, r.r3q, r.r3o, r.r3u, r.r3d))
        for ds in range(1, S):
            red[p, 2, ds].wait_send()
        red[p, 4] = net.remote(mine, mine, on_mate, (R2, p, 1), (FIN, p))
        go(red[p, 4])

    def flat(ref, w=None):
        v = ref[...] if w is None else ref[:, :, w]
        return v.reshape(I * R, v.shape[-1])

    def grad_down(h):
        def tile(w):
            r.gdn[w, :] = dot_tn(flat(r.activ, w), flat(r.cot)).astype(BF)

        tiles(F, tile, h, 2)
        reduce1(DN0 + h)

    def grad_up(h):
        def tile(w):
            r.gup[w, :] = dot_tn(flat(r.second, w), flat(r.actlow)).astype(BF)

        tiles(D, tile, h)
        if h == 1:
            reduce1(UP0)
            reduce1(UP1)

    def grad_out():
        r.gout[...] = dot_tn(flat(r.att), flat(r.mlow)).astype(BF)
        reduce1(OUT0)

    def grad_proj(*planes):
        def tile(w):
            x = flat(r.first, w)
            for n in planes:
                r.gqkv[n, w, :] = dot_tn(x, flat(r.pg.at[n])).astype(BF)

        tiles(D, tile)
        for n in planes:
            reduce1(Q0 + n)

    def middle_back(i):
        sum_got(3, i)

        def rows(w):
            unit, inv = norm_stats(r.middle[i, w, :])
            n2 = r.tot3[i, w, :].astype(F32)
            up = r.cot[i, w, :].astype(F32)
            g = up + norm_back(n2, unit, inv, r.g2[...])
            r.mgrad[i, w, :] = g
            r.mlow[i, w, :] = g.astype(BF)
            r.acc[1] += fold8(g)
            r.acc[4] += fold8(n2 * unit)
            r.acc[5] += fold8(n2)
            r.acc[7] += fold8(up)

        blocks(rows)

    def attention_back(i):
        k, v = all_keys(i)
        q = r.q[i].astype(F32)
        grad = dot_nt(r.mlow[i], r.wout[...])
        grad = grad.astype(BF).astype(F32)

        def head(h, total):
            mine = lane_head == h
            w = pl.ds(aligned(h * R, R), R)
            gh = jnp.where(mine, grad, 0.0).astype(BF)
            r.ost[w, :] = gh
            r.qst[w, :] = jnp.where(mine, q, 0.0).astype(BF)
            wg = dot_nt(gh, v)
            p = r.wts[i, w, :].astype(F32)
            pw = p * wg
            row_dot = jnp.sum(pw, axis=-1, keepdims=True)
            ds = ((pw - p * row_dot) * scale).astype(BF)
            r.dss[w, :] = ds
            return jnp.where(mine, dot(ds, k), total)

        dq = lax.fori_loop(0, heads, head, jnp.zeros((R, W), F32), unroll=True)
        r.acc[0, :, 0:W] += fold8(dq)
        r.pg[0, i] = dq.astype(BF)

    def key_grads(i):
        dk = dot_tn(r.dss[...], r.qst[...]).astype(BF)
        dv = dot_tn(r.wts[i], r.ost[...]).astype(BF)
        for b in range(C):
            r.dkv[b, i, 0] = dk[b * R : (b + 1) * R, :]
            r.dkv[b, i, 1] = dv[b * R : (b + 1) * R, :]
        key_send(i)

    back_mate, back_far, back_across = {}, {}, {}
    real = pl.ds(0, piece)

    def key_send(i):
        back_far[i] = net.remote(
            r.dkv.at[far, i, :, real], r.rxa.at[1, i, :, real], on_mate, (KM, 0), (KM, 0, i)
        )
        back_mate[i] = net.remote(
            r.dkv.at[mate, i, :, real], r.rxa.at[0, i, :, real], on_mate, (KM, 1), (KM, 1, i)
        )
        go(back_far[i], (KM, 0), r.rxb.at[:, :, real])
        go(back_mate[i], (KM, 1), r.rxb.at[:, :, real])

    def key_mid(i):
        back_far[i].wait_recv()
        for n in range(2):
            both = r.dkv[across, i, n].astype(F32) + r.rxa[1, i, n].astype(F32)
            r.rxa[1, i, n] = both.astype(BF)
        back_across[i] = net.remote(
            r.rxa.at[1, i, :, real], r.rxb.at[i, :, real], on_across, (KM, 2), (KM, 2, i)
        )
        go(back_across[i], (KM, 2), r.rxb.at[:, :, real])

    def key_end(i):
        back_mate[i].wait_recv()
        back_across[i].wait_recv()
        for n in range(2):
            both = r.dkv[c, i, n].astype(F32) + r.rxa[0, i, n].astype(F32)
            both = both + r.rxb[i, n].astype(F32)
            r.pg[1 + n, i] = both.astype(BF)
            if n == 1:
                r.acc[0, :, W : 2 * W] += fold8(both)

    def norm1_part(i, h):
        def tile(w):
            total = dot_nt(r.pg[0, i], r.wqkv[0, w, :])
            total = total + dot_nt(r.pg[1, i], r.wqkv[1, w, :])
            total = total + dot_nt(r.pg[2, i], r.wqkv[2, w, :])
            r.own4[i, :, w] = total.astype(BF)

        tiles(D, tile, h)

    puts = []

    def out_rows(i):
        sum_got(2, i)

        def rows(w):
            x = r.middle[i, w, :] + r.tot2[i, w, :].astype(F32) + r.bdn[...]
            r.middle[i, w, :] = x

        blocks(rows)
        put = net.local(r.middle.at[i, pl.ds(0, piece)], r.out_h.at[i])
        put.start()
        puts.append(put)

    def token_rows(i):
        sum_got(4, i)

        def rows(w):
            unit, inv = norm_stats(r.tok[i, w, :].astype(F32))
            n1 = r.tot4[i, w, :].astype(F32)
            g = r.mgrad[i, w, :] + norm_back(n1, unit, inv, r.g1[...])
            r.mgrad[i, w, :] = g
            r.acc[2] += fold8(n1 * unit)
            r.acc[3] += fold8(n1)

        blocks(rows)
        put = net.local(r.mgrad.at[i, pl.ds(0, piece)], r.gtok_h.at[i])
        put.start()
        puts.append(put)

    slot = s * C + c
    small = []

    def spread_small(mine, slots, key):
        slots[slot] = mine[...]
        for ds in range(S):
            for dc in range(C):
                if ds or dc:
                    to = (lax.rem(s + ds, S), lax.rem(c + dc, C), t)
                    copy = net.remote(mine, slots.at[slot], to, key, key)
                    copy.start()
        others = slots.at[pl.ds(0, S * C - 1)]
        small.append(net.remote(others, others, on_mate, key, key))

    def small_early():
        for k in (0, 1, 4, 5, 6, 7):
            r.sm[k : k + 1, :] = jnp.sum(r.acc[k], axis=0, keepdims=True)
        spread_small(r.sm, r.smx, SMA)

    def small_late():
        n = D // 4
        for k in range(2):
            total = jnp.sum(r.acc[2 + k], axis=0, keepdims=True)
            for q in range(4):
                r.smt[4 * k + q : 4 * k + q + 1, :] = total[:, q * n : (q + 1) * n]
        spread_small(r.smt, r.smtx, SMB)

    def finish():
        for full, home, pieces in (
            (r.fdn, r.fdn_h, (DN0, DN1)),
            (r.fup, r.fup_h, (UP0, UP1)),
            (r.fout, r.fout_h, (OUT0,)),
            (r.fqkv, r.fqkv_h, (Q0, K0, V0)),
        ):
            for p in pieces:
                red[p, 4].wait_recv()
            put = net.local(full, home)
            put.start()
            puts.append(put)
        for copy in small:
            copy.wait_recv()
        r.smo[...] = lax.fori_loop(1, S * C, lambda n, x: x + r.smx[n], r.smx[0])
        r.smto[...] = lax.fori_loop(1, S * C, lambda n, x: x + r.smtx[n], r.smtx[0])
        for put in puts:
            put.wait()
        for copy in (*sent, *small):
            copy.wait_send()
        for key, whole in last.items():
            drain(key, whole)
        owns, tots = (r.own1, r.own2, r.own3, r.own4), (r.tot1, r.tot2, r.tot3, r.tot4)

        @pl.when(edge)
        def _():
            for k in range(4):
                drain((SM, k + 1), owns[k].at[:, real])

        @pl.when(inner)
        def _():
            for k in range(4):
                drain((SM, k + 1), owns[k].at[:, real])
                drain((SE, k + 1), tots[k].at[:, real])

        assert len(net.sends) <= n_sends(d) and len(net.recvs) <= n_recvs(d)

    steps = {
        LN: first_norm, FW: pass_on, KP: key_part, QP: queries, KF: key_forward,
        AT: attention, P1: attn_part, SS: sum_start, SJ: sum_block, SM: sum_mid, SE: sum_end,
        MO: middle_of, FF: feed_forward, P3: norm2_part, P2: out_part, MB: middle_back,
        AB: attention_back, AC: key_grads, KM: key_mid, KE: key_end, P4: norm1_part, OR: out_rows,
        TR: token_rows, GD: grad_down, GU: grad_up, GO: grad_out, GQ: grad_proj, R2: reduce2,
        R3: reduce3, R4: reduce4, SMA: small_early, SMB: small_late, FIN: finish,
    }
    for step in ORDER:
        steps[step[0]](*step[1:])


def last_kernel(d, names, *refs):
    r = types.SimpleNamespace(**dict(zip(names, refs)))
    pairs = (
        (r.out_i, None, r.out_w, r.out_o),
        (r.fdn_i, r.fdn_v, r.fdn_w, r.fdn_o),
        (r.gtok_i, None, r.gtok_w, r.gtok_o),
        (r.fup_i, r.fup_v, r.fup_w, r.fup_o),
        (r.fqkv_i, r.fqkv_v, r.fqkv_w, r.fqkv_o),
        (r.fout_i, r.fout_v, r.fout_w, r.fout_o),
    )
    takes = []
    for n, (src, low, wide, dst) in enumerate(pairs):
        takes.append(pltpu.make_async_copy(src, wide if low is None else low, r.sem.at[n]))
        takes[-1].start()
    W, D, F = d.local, d.width, d.hidden
    r.bqv_o[0:1, :] = r.small[0:1, 0:W]
    r.bqv_o[1:2, :] = r.small[0:1, W : 2 * W]
    r.bout_o[...] = r.small[1:2, :]
    r.g2_o[...] = r.small[4:5, :]
    r.b2_o[...] = r.small[5:6, :]
    r.bup_o[...] = r.small[6:7, 0:F]
    r.bdn_o[...] = r.small[7:8, :]
    n4 = D // 4
    for q in range(4):
        w = pl.ds(q * n4, n4)
        r.g1_o[:, w] = r.late[q : q + 1, :]
        r.b1_o[:, w] = r.late[4 + q : 5 + q, :]
    puts = []

    def put(src, dst):
        puts.append(pltpu.make_async_copy(src, dst, r.sem.at[len(pairs) + len(puts)]))
        puts[-1].start()

    def widen(a, b):
        m = 64 if a.shape[0] % 64 == 0 else RB

        def step(k, _):
            w = span(k, m)
            b[w, :] = a[w, :].astype(F32)
            return 0

        lax.fori_loop(0, a.shape[0] // m, step, 0)

    for n, (src, low, wide, dst) in enumerate(pairs):
        takes[n].wait()
        if low is None:
            put(wide, dst)
        elif len(low.shape) == 3:
            for k in range(low.shape[0]):
                widen(low.at[k], wide.at[k])
                put(wide.at[k], dst.at[k])
        else:
            rows = low.shape[0] // (2 if low.shape[0] % 128 == 0 else 1)
            for k in range(low.shape[0] // rows):
                w = pl.ds(k * rows, rows)
                widen(low.at[w], wide.at[w])
                put(wide.at[w], dst.at[w])
    for copy in puts:
        copy.wait()


def call_last(d, out, gtok, fqkv, fout, fup, fdn, small, late):
    I, D, W, F = d.images, d.width, d.local, d.hidden
    arr = jax.ShapeDtypeStruct
    ins = dict(out_i=out, gtok_i=gtok, fqkv_i=fqkv, fout_i=fout, fup_i=fup, fdn_i=fdn)
    ins.update(small=small, late=late)
    outs = dict(out_o=arr(out.shape, F32), gtok_o=arr(gtok.shape, F32))
    outs.update(fqkv_o=arr(fqkv.shape, F32), fout_o=arr(fout.shape, F32))
    outs.update(fup_o=arr(fup.shape, F32), fdn_o=arr(fdn.shape, F32))
    outs.update(bqv_o=arr((2, W), F32), bout_o=arr((1, D), F32), g1_o=arr((1, D), F32))
    outs.update(b1_o=arr((1, D), F32), g2_o=arr((1, D), F32), b2_o=arr((1, D), F32))
    outs.update(bup_o=arr((1, F), F32), bdn_o=arr((1, D), F32))
    vm = lambda a, t: pltpu.VMEM(a.shape, t)
    scratch = dict(fqkv_v=vm(fqkv, BF), fout_v=vm(fout, BF), fup_v=vm(fup, BF), fdn_v=vm(fdn, BF))
    scratch.update(fqkv_w=vm(fqkv, F32), fout_w=vm(fout, F32), fup_w=vm(fup, F32))
    scratch.update(fdn_w=vm(fdn, F32), out_w=vm(out, F32), gtok_w=vm(gtok, F32))
    scratch.update(sem=pltpu.SemaphoreType.DMA((18,)))
    vmem = pl.BlockSpec(memory_space=pltpu.VMEM)
    hbm = pl.BlockSpec(memory_space=pl.ANY)
    return pl.pallas_call(
        functools.partial(last_kernel, d, (*ins, *outs, *scratch)),
        out_shape=tuple(outs.values()),
        in_specs=[hbm] * 6 + [vmem] * 2,
        out_specs=(hbm,) * 6 + (vmem,) * 8,
        scratch_shapes=list(scratch.values()),
        compiler_params=pltpu.CompilerParams(vmem_limit_bytes=60 * 2**20),
        name="results",
    )(*ins.values())


def call_kernel(d, ins):
    scratch = scratch_of(d)
    I, D, W, F = d.images, d.width, d.local, d.hidden
    vmem = pl.BlockSpec(memory_space=pltpu.VMEM)
    hbm = pl.BlockSpec(memory_space=pl.ANY)
    arr = jax.ShapeDtypeStruct
    outs = dict(
        out_h=arr((I, d.piece, D), F32),
        gtok_h=arr((I, d.piece, D), F32),
        fqkv_h=arr((3, d.part, W), BF),
        fout_h=arr((W, d.part), BF),
        fup_h=arr((d.part, F), BF),
        fdn_h=arr((F, d.part), BF),
        smo=arr((8, D), F32),
        smto=arr((8, D // 4), F32),
    )
    names = (*ins, *outs, *scratch)
    return pl.pallas_call(
        functools.partial(body_kernel, d, names),
        out_shape=tuple(outs.values()),
        in_specs=[hbm] * 15,
        out_specs=(hbm,) * 6 + (vmem,) * 2,
        scratch_shapes=list(scratch.values()),
        compiler_params=pltpu.CompilerParams(
            collective_id=0, has_side_effects=True, vmem_limit_bytes=67043328
        ),
        name="encoder_layer",
    )(*ins.values())


def body(mesh, tokens, pad_mask, ln1_gain, ln1_shift, w_qkv, b_qv, w_out, b_out, ln2_gain, ln2_shift, w_up, b_up, w_down, b_down, cotangent):
    d = dims_of(mesh, tokens.shape, w_out.shape, w_up.shape)
    row = lambda v: v.reshape(1, -1)
    ins = dict(
        tok_h=tokens,
        cot_h=cotangent,
        wqkv_h=w_qkv,
        wout_h=w_out,
        wup_h=w_up,
        wdn_h=w_down,
        mask_h=pad_mask,
        g1_h=row(ln1_gain),
        b1_h=row(ln1_shift),
        bqv_h=b_qv,
        bout_h=row(b_out),
        g2_h=row(ln2_gain),
        b2_h=row(ln2_shift),
        bup_h=row(b_up),
        bdn_h=row(b_down),
    )
    out, gtok, gqkv, gout, gup, gdn, bqv, bout, g1, b1, g2, b2, bup, bdn = call_last(
        d, *call_kernel(d, ins)
    )
    flat = lambda v: v.reshape(-1)
    return (
        out, gtok, gqkv, bqv, gout, flat(bout), flat(g1), flat(b1), flat(g2), flat(b2), gup,
        flat(bup), gdn, flat(bdn),
    )


def solution(mesh):
    return jax.shard_map(
        functools.partial(body, mesh),
        mesh=mesh,
        in_specs=(
            P("shard", "ctx", None),
            P("shard", "ctx"),
            P(),
            P(),
            P(None, "shard", "tp"),
            P(None, "tp"),
            P("tp", "shard"),
            P(),
            P(),
            P(),
            P("shard", "tp"),
            P("tp"),
            P("tp", "shard"),
            P(),
            P("shard", "ctx", None),
        ),
        out_specs=(
            P("shard", "ctx", None),
            P("shard", "ctx", None),
            P(None, "shard", "tp"),
            P(None, "tp"),
            P("tp", "shard"),
            P(),
            P(),
            P(),
            P(),
            P(),
            P("shard", "tp"),
            P("tp"),
            P("tp", "shard"),
            P(),
        ),
        check_vma=False,
    )
```
